32 devices in a mesh: dom: 8 (over z, y), sub: 4 (over x, core).
Axes of the slice: x: 2, y: 2, z: 4, core: 2. Of those that a mesh axis runs over, the one named last changes fastest.
Arguments:
- positions: float32 [2048, 3, 256], P(('dom', 'sub')), may hold values from -6 to 6
- time_bins: int32 [2048, 256], P(('dom', 'sub')), may hold values from 0 to 5
- home_groups: int32 [2048], P(('dom', 'sub')), may hold values from 0 to 63
- targets: int32 [2048, 4], P(('dom', 'sub')), may hold values from -1 to 7, as said below
- target_groups: int32 [2048, 4], P(('dom', 'sub')), may hold values from 0 to 63
- node_pos: float32 [3, 131072], P(None, ('dom', 'sub')), may hold values from -6 to 6
- node_mass: float32 [131072], P(('dom', 'sub')), may hold values from 0.2 to 2
- node_lists: int32 [512, 256], P('dom'), may hold values from 0 to 16383
- list_counts: int32 [512], P('dom'), may hold values from 64 to 256, as said below
Outputs:
- forces: float32 [2048, 3, 256], P(('dom', 'sub'))
The draws below stay inside these ranges and needn't reach their ends.
Inputs may be any that keep to these rules, and one draw needn't show every extreme that they name: `targets`: row b names the remote domains that block b visits, each at most once and never its own domain b // 256; -1 marks an unused entry, in any column. The rows of one device name one domain at most 32 times, and some device names some domain exactly 32 times in every draw. The rows of one domain's 4 devices together name one domain at most 64 times, and this is reached in every draw. `list_counts`: each domain has at least one list with all 256 entries valid.
All inputs are finite; a program needn't handle non-finite values.
Results may differ from the reference program's by a relative error of at most 0.0003.
Values sent between devices are 32-bit elements; how exact they have to be, the bound alone decides.
A program may use at most 128 MiB of HBM per device.

```python
import math
import jax
import jax.numpy as jnp
from jax import lax

BLOCK = 256
BLK_DEV = 64
TOP = 4
LIST = 256
GROUPS = 64
NODE_DEV = 4096
BINS = 6
CUR_BIN = 2
BLOCKS = 2048
NODES = 131072
CAP = 32
CAP_ROW = 64
N_DOM = 8
N_SUB = 4


def draw_list_counts(key, part):
    count_key = jax.random.fold_in(key, 11)
    full_key = jax.random.fold_in(key, 12)
    counts = jax.random.randint(count_key, (N_DOM, GROUPS), LIST // 4, LIST + 1)
    full_list = jax.random.randint(full_key, (N_DOM,), 0, GROUPS)
    counts = jnp.where(jnp.arange(GROUPS)[None, :] == full_list[:, None], LIST, counts)
    return counts.reshape(N_DOM * GROUPS).astype(jnp.int32)


def draw_targets(key, part):
    hot_key = jax.random.fold_in(key, 21)
    order_key = jax.random.fold_in(key, 22)
    level_key = jax.random.fold_in(key, 23)
    wish_key = jax.random.fold_in(key, 24)
    block_key = jax.random.fold_in(key, 25)
    column_key = jax.random.fold_in(key, 26)
    hot_domain = jax.random.randint(hot_key, (), 0, N_DOM)
    domain_ids = jnp.arange(N_DOM, dtype=jnp.int32)
    orders = jax.vmap(lambda one_key: jax.random.permutation(one_key, N_SUB))(jax.random.split(order_key, N_DOM))
    levels = jax.random.randint(level_key, (N_DOM, N_SUB, 1), 0, 4)
    wishes = jnp.minimum(CAP, jax.random.randint(wish_key, (N_DOM, N_SUB, N_DOM), 0, CAP + 1) * levels // 2)
    wishes = jnp.where(domain_ids[None, None, :] == hot_domain, CAP, wishes)
    wishes = jnp.where(domain_ids[:, None, None] == domain_ids[None, None, :], 0, wishes).astype(jnp.int32)
    rotation = (hot_domain + domain_ids) % N_DOM
    unrotate = (domain_ids - hot_domain) % N_DOM
    budget = BLK_DEV * TOP

    def row_counts(row_wishes, row_order):

        def advance(already, position):
            wanted = jnp.minimum(row_wishes[row_order[position]], CAP_ROW - already)
            turned = wanted[rotation]
            before = jnp.cumsum(turned) - turned
            granted = jnp.maximum(jnp.minimum(turned, budget - before), 0)[unrotate]
            return (already + granted, granted)
        _, granted = lax.scan(advance, jnp.zeros((N_DOM,), jnp.int32), jnp.arange(N_SUB))
        return jnp.zeros((N_SUB, N_DOM), jnp.int32).at[row_order].set(granted)
    counts = jax.vmap(row_counts)(wishes, orders).reshape(N_DOM * N_SUB, N_DOM)
    tickets = jnp.arange(budget, dtype=jnp.int32)

    def device_table(device_counts, shuffle_key, order_keys):
        boundaries = jnp.cumsum(device_counts)
        ticket_domain = jnp.sum((boundaries[None, :] <= tickets[:, None]).astype(jnp.int32), axis=1)
        ticket_domain = jnp.where(tickets < boundaries[-1], ticket_domain, -1)
        assigned = ticket_domain.reshape(TOP, BLK_DEV).T
        assigned = assigned[jax.random.permutation(shuffle_key, BLK_DEV)]
        column_orders = jax.vmap(lambda one_key: jax.random.permutation(one_key, TOP))(jax.random.split(order_keys, BLK_DEV))
        return jnp.take_along_axis(assigned, column_orders, axis=1)
    device_total = N_DOM * N_SUB
    tables = jax.vmap(device_table)(counts, jax.random.split(block_key, device_total), jax.random.split(column_key, device_total))
    return tables.reshape(device_total * BLK_DEV, TOP).astype(jnp.int32)


def set_ends(array, own_key, smallest, largest):
    dims = array.shape
    index_at = [jax.random.randint(jax.random.fold_in(own_key, axis), (), 0, dims[axis]) for axis in range(len(dims))]
    array = array.at[tuple(index_at)].set(smallest)
    longest = dims.index(max(dims))
    index_at[longest] = (index_at[longest] + 1) % dims[longest]
    return array.at[tuple(index_at)].set(largest)


def shard_levels(stream_key, shape, cuts, smallest, largest):
    factor_of, own = 1.0, jax.random.fold_in(stream_key, 6)
    for axis_at, blocks in cuts:
        draws = jnp.exp(jax.random.uniform(jax.random.fold_in(own, axis_at), (blocks,), jnp.float32, smallest / len(cuts), largest / len(cuts)))
        factor_of = factor_of * jnp.repeat(draws, shape[axis_at] // blocks).reshape([-1 if axis == axis_at else 1 for axis in range(len(shape))])
    return factor_of


def bell_draw(key, extent, scale, most, pieces=(), kind=jnp.bfloat16):
    values = jax.random.normal(key, extent, jnp.float32) * scale
    if len(pieces) > 0:
        values = shard_levels(key, extent, pieces, -0.22, 0.18) * values
    return jnp.clip(values, min=-most, max=most).astype(kind)


def setup_inputs(seed: int = 0) -> dict:
    seeds = jax.random.split(jax.random.key(seed), 10)
    positions = bell_draw(seeds[0], (BLOCKS, 3, BLOCK), 1.0, 6.0, ((0, 32),), jnp.float32)
    time_bins = set_ends(jax.random.randint(seeds[1], (BLOCKS, BLOCK), 0, BINS), jax.random.fold_in(seeds[1], 1), 0, BINS - 1).astype(jnp.int32)
    home_groups = set_ends(jax.random.randint(seeds[2], (BLOCKS,), 0, GROUPS), jax.random.fold_in(seeds[2], 1), 0, GROUPS - 1).astype(jnp.int32)
    targets = draw_targets(jax.random.fold_in(seeds[9], 71), 0)
    target_groups = set_ends(jax.random.randint(seeds[4], (BLOCKS, TOP), 0, GROUPS), jax.random.fold_in(seeds[4], 1), 0, GROUPS - 1).astype(jnp.int32)
    node_pos = bell_draw(seeds[5], (3, NODES), 1.0, 6.0, ((1, 32),), jnp.float32)
    node_mass = jnp.clip(jnp.exp(math.log(2.0) - 2.3025851 * jax.random.uniform(seeds[6], (NODES,), jnp.float32) ** shard_levels(seeds[6], (NODES,), ((0, 32),), -0.2, 0.2)), 0.2, 2.0)
    node_lists = set_ends(jax.random.randint(seeds[7], (N_DOM * GROUPS, LIST), 0, NODE_DEV * N_SUB), jax.random.fold_in(seeds[7], 1), 0, (NODE_DEV * N_SUB) - 1).astype(jnp.int32)
    list_counts = draw_list_counts(jax.random.fold_in(seeds[9], 71), 0)
    return dict(positions=positions, time_bins=time_bins, home_groups=home_groups, targets=targets, target_groups=target_groups, node_pos=node_pos, node_mass=node_mass, node_lists=node_lists, list_counts=list_counts)


soften_sq = 0.04
gauss_slope = 1.1283791670955126

def short_pull(sink_pos, source_pos, source_mass):
    offset = sink_pos[:, None, :] - source_pos[:, :, None]
    range_sq = lax.optimization_barrier(jnp.sum(offset * offset, axis=0)) + soften_sq
    distance = jnp.sqrt(range_sq)
    scaled = distance * 0.5
    factor = lax.erfc(scaled) + gauss_slope * scaled * jnp.exp(-scaled * scaled)
    weight = source_mass[:, None] * factor / (range_sq * distance)
    return -lax.optimization_barrier(jnp.sum(offset * weight[None, :, :], axis=1))

def reference(positions, time_bins, home_groups, targets, target_groups, node_pos, node_mass, node_lists, list_counts):
    per_domain = BLK_DEV * N_SUB
    node_count = NODE_DEV * N_SUB
    block_ids = jnp.arange(BLOCKS, dtype=jnp.int32)
    home_domain = block_ids // per_domain
    visit_domain = jnp.concatenate([home_domain[:, None], jnp.maximum(targets, 0)], axis=1).astype(jnp.int32)
    visit_group = jnp.concatenate([home_groups[:, None], target_groups], axis=1).astype(jnp.int32)
    visit_alive = jnp.concatenate([jnp.ones((BLOCKS, 1), jnp.float32), (targets >= 0).astype(jnp.float32)], axis=1)
    list_rows = visit_domain * GROUPS + visit_group
    entry_ids = jnp.arange(LIST, dtype=jnp.int32)

    def one_visit(sink_pos, list_row, domain_id, is_alive):
        node_index = node_lists[list_row] + domain_id * node_count
        node_weight = node_mass[node_index] * (entry_ids < list_counts[list_row]).astype(jnp.float32) * is_alive
        return short_pull(sink_pos, node_pos[:, node_index], node_weight)

    def one_block(sink_pos, block_rows, block_domains, block_alive):
        pulls = jax.vmap(one_visit, in_axes=(None, 0, 0, 0))(sink_pos, block_rows, block_domains, block_alive)
        return lax.optimization_barrier(jnp.sum(pulls, axis=0))

    def one_group(operands):
        return jax.vmap(one_block)(*operands)
    grouped = lax.map(one_group, (positions.reshape(BLOCKS // 8, 8, 3, BLOCK), list_rows.reshape(BLOCKS // 8, 8, TOP + 1), visit_domain.reshape(BLOCKS // 8, 8, TOP + 1), visit_alive.reshape(BLOCKS // 8, 8, TOP + 1)))
    summed = grouped.reshape(BLOCKS, 3, BLOCK)
    active = (time_bins <= CUR_BIN).astype(jnp.float32)
    return summed * active[:, None, :]
```

```python
import functools
import math

import jax
import jax.numpy as jnp
from jax import lax
from jax.experimental import pallas as pl
from jax.experimental.pallas import tpu as pltpu
from jax.sharding import PartitionSpec as P

CUR_BIN = 2
SOFTEN_SQ = 0.04
LANES = 128
SCALE = math.sqrt(math.log2(math.e) / 4)
KAPPA = 0.5033782057491644
LEAD = 1.0644227815066034
POLY = (
    0.0006822818085192818,
    0.6891780368303475,
    -0.07494018001023989,
    -0.03418881002810906,
    0.008589076872810486,
)
MASS_SCALE = LEAD * SCALE / math.sqrt(math.pi)
MESH = pl.DeviceIdType.MESH
TILE = 144
PAIR = 2


def bf16_pieces(value):
    pieces = []
    for _ in range(3):
        mantissa, exponent = math.frexp(value)
        piece = math.ldexp(round(mantissa * 256), exponent - 8)
        pieces.append(piece)
        value -= piece
    return tuple(pieces)


SOFT = bf16_pieces(SOFTEN_SQ * SCALE * SCALE)


def gather_kernel(nodes, ids, counts, out):
    sharers, _, table_rows, _ = nodes.shape
    rows = ids.shape[0]
    index = ids[...]
    high = index >> 7
    low = index & (LANES - 1)
    for owner in range(sharers):

        def one(step, found):
            for sub_step in range(2):
                row = step * 2 + sub_step
                here = high == owner * table_rows + row
                fresh = []
                for feature in range(4):
                    line = jnp.broadcast_to(nodes[owner, feature, pl.ds(row, 1), :], (rows, LANES))
                    value = jnp.take_along_axis(line, low, axis=1, mode="promise_in_bounds")
                    fresh.append(jnp.where(here, value, found[feature]))
                found = tuple(fresh)
            return found

        if owner == 0:
            found = (jnp.zeros((rows, LANES), jnp.float32),) * 4
        found = lax.fori_loop(0, table_rows // 2, one, found)
    lane = lax.broadcasted_iota(jnp.int32, (rows, LANES), 1)
    half = lax.broadcasted_iota(jnp.int32, (rows, LANES), 0) & 1
    valid = (half * LANES + lane) < counts[...]
    mass = jnp.where(valid, found[3] * MASS_SCALE, 0.0)
    values = tuple(found[f] * SCALE for f in range(3)) + (mass,)
    for row in range(rows):
        for feature in range(4):
            at = (row % 2) * 4 + feature
            out[row // 2, at : at + 1, :] = values[feature][row : row + 1, :]


def share_nodes_kernel(own, out, send_sem, recv_sem):
    sharers = lax.axis_size("sub")
    place = lax.axis_index("sub")
    barrier = pltpu.get_barrier_semaphore()
    others = [lax.rem(place + k, sharers) for k in range(1, sharers)]
    for other in others:
        pl.semaphore_signal(barrier, inc=1, device_id={"sub": other}, device_id_type=MESH)
    pl.semaphore_wait(barrier, sharers - 1)
    copies = []
    for k, other in enumerate(others):
        copy = pltpu.make_async_remote_copy(
            src_ref=own,
            dst_ref=out.at[place],
            send_sem=send_sem.at[k],
            recv_sem=recv_sem.at[k],
            device_id={"sub": other},
            device_id_type=MESH,
        )
        copy.start()
        copies.append(copy)
    out[place] = own[...]
    for copy in copies:
        copy.wait()


def share_tables_kernel(own, out, send_sem, recv_sem, near_send, near_recv):
    half = lax.axis_size("sub") // 2
    chips = lax.axis_size("dom") * half
    domain, place = lax.axis_index("dom"), lax.axis_index("sub")
    core = lax.rem(place, 2)
    chip = domain * half + place // 2
    sibling = {"sub": place + 1 - 2 * core}

    def device(k):
        there = lax.rem(chip + k, chips)
        return {"dom": there // half, "sub": lax.rem(there, half) * 2 + core}

    def slot(k):
        return lax.rem(chip + chips - k, chips) * 2 + core

    barrier = pltpu.get_barrier_semaphore()
    pl.semaphore_signal(barrier, inc=1, device_id=sibling, device_id_type=MESH)

    @pl.loop(1, chips)
    def _(k):
        pl.semaphore_signal(barrier, inc=1, device_id=device(k), device_id_type=MESH)

    pl.semaphore_wait(barrier, chips)

    def far(k, at):
        return pltpu.make_async_remote_copy(
            src_ref=own,
            dst_ref=out.at[at],
            send_sem=send_sem.at[k],
            recv_sem=recv_sem.at[k],
            device_id=device(k),
            device_id_type=MESH,
        )

    def near(k, source):
        return pltpu.make_async_remote_copy(
            src_ref=source,
            dst_ref=out.at[slot(k)],
            send_sem=near_send.at[k],
            recv_sem=near_recv.at[k],
            device_id=sibling,
            device_id_type=MESH,
        )

    @pl.loop(1, chips)
    def _(k):
        far(k, slot(0)).start()

    near(0, own).start()
    out[slot(0)] = own[...]

    @pl.loop(1, chips)
    def _(k):
        far(k, slot(k)).wait_recv()
        near(k, out.at[slot(k)]).start()

    near(0, own).wait()

    @pl.loop(1, chips)
    def _(k):
        far(k, slot(0)).wait_send()
        near(k, out.at[slot(k)]).wait()


def split(value):
    high = value.astype(jnp.bfloat16).astype(jnp.float32)
    rest = value - high
    middle = rest.astype(jnp.bfloat16).astype(jnp.float32)
    return value, rest, rest - middle


def radial(range_sq):
    near = lax.rsqrt(range_sq)
    fall = 1.0 / (range_sq * jnp.exp2(range_sq))
    z = 1.0 / (near + KAPPA)
    poly = z * POLY[-1] + POLY[-2]
    for coefficient in POLY[-3::-1]:
        poly = poly * z + coefficient
    return (poly + near) * fall


def pull_kernel(
    share, stride, rows, counts, active_counts, pos, ranks, table, out,
    items, chosen, sinks, totals, later_range, later_weight, later_nodes,
):
    blocks = active_counts.shape[0]
    visits = rows.shape[0] // blocks
    width = pos.shape[2]
    tiles = sinks.shape[0] // blocks
    spare = tiles * blocks
    f32, bf16 = jnp.float32, jnp.bfloat16
    sub8 = lax.broadcasted_iota(jnp.int32, (8, width), 0)
    axis8 = sub8 & 3
    by_rows = (((1,), (1,)), ((), ()))
    order = lax.broadcasted_iota(jnp.int32, (TILE, width), 0)
    lane48 = lax.broadcasted_iota(jnp.int32, (TILE, 48), 1)
    soft_high, soft_rest, soft_last = SOFT
    soft = jnp.where(
        lane48 == 11,
        soft_high,
        jnp.where(lane48 == 27, soft_rest, jnp.where(lane48 == 43, soft_last, 0.0)),
    )

    def axes(first, second, third, fourth, at):
        return jnp.where(at == 0, first, jnp.where(at == 1, second, jnp.where(at == 2, third, fourth)))

    def prepare(block):
        line = [
            jnp.broadcast_to(pos[axis, pl.ds(block, 1), :] * SCALE, (8, width))
            for axis in range(3)
        ]
        norm = line[0] * line[0] + line[1] * line[1] + line[2] * line[2]
        pieces = split(axes(line[0], line[1], line[2], 0.0, axis8) * -2.0)
        norms = split(norm)
        parts = []
        for k in range(3):
            tail = jnp.where(sub8 == 7, norms[k], 1.0 if k == 0 else 0.0)
            parts.append(pieces[k])
            parts.append(jnp.where(sub8 < 3, pieces[k], jnp.where(sub8 == 3, 0.0, tail)))
        wide = jnp.concatenate(parts, axis=0).astype(bf16)
        rank = ranks[pl.ds(block, 1), :]

        def fill(tile):
            at = tile * blocks + block
            pick = jnp.where(order == rank - tile * TILE, 1.0, 0.0).astype(bf16)
            chosen[at] = pick
            held = lax.dot_general(pick, wide, by_rows, preferred_element_type=f32)
            sinks[at] = (held + soft).astype(bf16)
            totals[at] = jnp.zeros((TILE, 16), f32)

        fill(0)
        for tile in range(1, tiles):
            pl.when(active_counts[block] > tile * TILE)(functools.partial(fill, tile))

    def list_items(block, at):
        for visit in range(visits):
            row = rows[block * visits + visit]
            safe = jnp.maximum(row, 0)
            line = safe // share * stride + safe % share * 8
            count = jnp.where(row >= 0, counts[safe], 0)
            for half in range(2):
                for tile in range(tiles):
                    items[at] = (tile * blocks + block) * 65536 + line + half * 4
                    need = count > half * LANES
                    if tile > 0:
                        need = jnp.logical_and(need, active_counts[block] > tile * TILE)
                    at = at + jnp.where(need, 1, 0)
        return at

    def first(step, at):
        for k in range(4):
            block = step * 4 + k
            prepare(block)
            at = list_items(block, at)
        return at

    sinks[spare] = soft.astype(bf16)
    totals[spare] = jnp.zeros((TILE, 16), f32)
    number = lax.fori_loop(0, blocks // 4, first, jnp.int32(0))
    for k in range(5 * PAIR):
        items[number + k] = spare * 65536

    sub = lax.broadcasted_iota(jnp.int32, (8, LANES), 0)
    axis = sub & 3

    def begin(item):
        code = items[item]
        line = code & 65535
        at = code >> 16
        row = [jnp.broadcast_to(table[pl.ds(line + f, 1), :], (8, LANES)) for f in range(4)]
        norm = row[0] * row[0] + row[1] * row[1] + row[2] * row[2]
        flat = axes(row[0], row[1], row[2], row[3], axis)
        pieces = split(flat)
        norms = split(norm)
        tail = jnp.where(
            sub == 4, norms[0], jnp.where(sub == 5, norms[1], jnp.where(sub == 6, norms[2], 1.0))
        )
        group = jnp.concatenate(
            [
                jnp.where(sub < 4, pieces[0], pieces[1]),
                jnp.where(sub < 3, pieces[2], tail),
            ],
            axis=0,
        ).astype(bf16)
        weighted = split(jnp.where(axis == 3, flat, flat * row[3]))
        moment = jnp.concatenate(
            [
                jnp.where(sub < 4, weighted[0], weighted[1]),
                jnp.where(sub < 4, weighted[2], 0.0),
            ],
            axis=0,
        ).astype(bf16)
        range_sq = jnp.dot(
            sinks[at], jnp.concatenate([group] * 3, axis=0), preferred_element_type=f32
        )
        return range_sq, jnp.concatenate([moment] * 2, axis=1)

    def weigh(range_sq):
        weight = radial(range_sq)
        high = weight.astype(bf16)
        low = (weight - high.astype(f32)).astype(bf16)
        return jnp.concatenate([high, low], axis=1)

    def gather(weight, moment):
        return lax.dot_general(weight, moment, by_rows, preferred_element_type=f32)

    def add(item, pull):
        at = items[item] >> 16
        totals[at] += pull

    for k in range(PAIR):
        later_range[k], later_nodes[k] = begin(k)
        later_weight[k] = jnp.zeros(later_weight.shape[1:], bf16)
        later_nodes[PAIR + k] = jnp.zeros(later_nodes.shape[1:], bf16)

    def main(step, carry):
        base = step * (2 * PAIR)
        before = [gather(later_weight[k], later_nodes[PAIR + k]) for k in range(PAIR)]
        middle = [begin(base + PAIR + k) for k in range(PAIR)]
        now = [gather(weigh(later_range[k]), later_nodes[k]) for k in range(PAIR)]
        for k in range(PAIR):
            add(jnp.where(step > 0, base - PAIR + k, number), before[k])
        after = [begin(base + 2 * PAIR + k) for k in range(PAIR)]
        for k in range(PAIR):
            later_weight[k] = weigh(middle[k][0])
            later_nodes[PAIR + k] = middle[k][1]
        for k in range(PAIR):
            add(base + k, now[k])
        for k in range(PAIR):
            later_range[k], later_nodes[k] = after[k]
        return carry

    groups = (number + PAIR - 1) // PAIR
    lax.fori_loop(0, groups // 2 + 1, main, 0)

    unit = lax.broadcasted_iota(jnp.int32, (8, 16), 1) & 3
    turn = jnp.where(
        (unit == lax.broadcasted_iota(jnp.int32, (8, 16), 0))
        & (lax.broadcasted_iota(jnp.int32, (8, 16), 1) < 12),
        1.0,
        0.0,
    ).astype(bf16)

    def spread(at):
        flat = sum(
            lax.dot_general(turn, piece.astype(bf16), by_rows, preferred_element_type=f32)
            for piece in split(totals[at])
        )
        pieces = jnp.concatenate(split(flat), axis=0).astype(bf16)
        laid = jnp.dot(pieces, chosen[at], preferred_element_type=f32)
        return laid[0:8] + laid[8:16] + laid[16:24]

    def store(block, laid):
        for axis in range(3):
            there = pos[axis, pl.ds(block, 1), :] * SCALE
            out[axis, pl.ds(block, 1), :] = laid[axis : axis + 1] - laid[3:4] * there

    def last(step, carry):
        for k in range(4):
            block = step * 4 + k
            store(block, spread(block))
        for k in range(4):
            block = step * 4 + k

            @pl.when(active_counts[block] > TILE)
            def _():
                laid = spread(block)
                for tile in range(1, tiles):
                    extra = spread(tile * blocks + block)
                    live = active_counts[block] > tile * TILE
                    laid = laid + jnp.where(live, extra, 0.0)
                store(block, laid)

        return carry

    lax.fori_loop(0, blocks // 4, last, 0)


def local(
    positions,
    time_bins,
    home_groups,
    targets,
    target_groups,
    node_pos,
    node_mass,
    node_lists,
    list_counts,
):
    domains = lax.axis_size("dom")
    sharers = lax.axis_size("sub")
    domain = lax.axis_index("dom")
    place = lax.axis_index("sub")
    blocks, most_visits = targets.shape
    width = positions.shape[2]
    groups, length = node_lists.shape
    share = groups // sharers
    halves = length // LANES

    own = jnp.concatenate([node_pos, node_mass[None, :]], axis=0).reshape(4, -1, LANES)
    vmem = pl.BlockSpec(memory_space=pltpu.VMEM)
    dma = pltpu.SemaphoreType.DMA
    domain_nodes = pl.pallas_call(
        share_nodes_kernel,
        out_shape=jax.ShapeDtypeStruct((sharers,) + own.shape, jnp.float32),
        in_specs=[vmem],
        out_specs=vmem,
        scratch_shapes=[dma((sharers - 1,)), dma((sharers - 1,))],
        compiler_params=pltpu.CompilerParams(collective_id=0, has_side_effects=True),
    )(own)

    ids = lax.dynamic_slice_in_dim(node_lists, place * share, share, 0).reshape(-1, LANES)
    own_counts = lax.dynamic_slice_in_dim(list_counts, place * share, share, 0)
    tables = pl.pallas_call(
        gather_kernel,
        out_shape=jax.ShapeDtypeStruct((share, 8, LANES), jnp.float32),
        in_specs=[vmem] * 3,
        out_specs=vmem,
    )(domain_nodes, ids, jnp.repeat(own_counts, halves)[:, None])
    tail = jnp.zeros((8, LANES), jnp.float32)
    tail = tail.at[0, :share].set(own_counts.astype(jnp.float32))
    sent = jnp.concatenate([tables.reshape(share * 8, LANES), tail], axis=0)
    chips = domains * sharers // 2
    table = pl.pallas_call(
        share_tables_kernel,
        out_shape=jax.ShapeDtypeStruct((domains * sharers,) + sent.shape, jnp.float32),
        in_specs=[vmem],
        out_specs=vmem,
        scratch_shapes=[dma((chips,))] * 4,
        compiler_params=pltpu.CompilerParams(
            collective_id=1, has_side_effects=True, vmem_limit_bytes=48 * 1024 * 1024
        ),
    )(sent)
    counts = table[:, share * 8, :share].reshape(-1).astype(jnp.int32)

    is_active = time_bins <= CUR_BIN
    active_counts = jnp.sum(is_active.astype(jnp.int32), axis=1)
    lower = jnp.arange(width)[:, None] <= jnp.arange(width)[None, :]
    running = jnp.dot(
        is_active.astype(jnp.bfloat16),
        lower.astype(jnp.bfloat16),
        preferred_element_type=jnp.float32,
    ).astype(jnp.int32)
    ranks = jnp.where(is_active, running - 1, -1)
    rows = jnp.concatenate(
        [
            (domain * groups + home_groups)[:, None],
            jnp.where(targets >= 0, targets * groups + target_groups, -1),
        ],
        axis=1,
    ).reshape(-1)

    visits = most_visits + 1
    tiles = -(-width // TILE)
    stride = table.shape[1]
    spare = tiles * blocks
    scratch = [
        pltpu.SMEM((blocks * visits * halves * tiles + 16 * PAIR,), jnp.int32),
        pltpu.VMEM((spare, TILE, width), jnp.bfloat16),
        pltpu.VMEM((spare + 1, TILE, 48), jnp.bfloat16),
        pltpu.VMEM((spare + 1, TILE, 16), jnp.float32),
        pltpu.VMEM((PAIR, TILE, LANES), jnp.float32),
        pltpu.VMEM((PAIR, TILE, 2 * LANES), jnp.bfloat16),
        pltpu.VMEM((2 * PAIR, 16, 2 * LANES), jnp.bfloat16),
    ]
    smem = pl.BlockSpec(memory_space=pltpu.SMEM)
    forces = pl.pallas_call(
        functools.partial(pull_kernel, share, stride),
        out_shape=jax.ShapeDtypeStruct((3, blocks, width), jnp.float32),
        in_specs=[smem] * 3 + [vmem] * 3,
        out_specs=vmem,
        scratch_shapes=scratch,
        compiler_params=pltpu.CompilerParams(vmem_limit_bytes=60 * 1024 * 1024),
    )(
        rows,
        counts,
        active_counts,
        jnp.transpose(positions, (1, 0, 2)),
        ranks,
        table.reshape(-1, LANES),
    )
    return jnp.transpose(forces, (1, 0, 2))


def solution(mesh):
    return jax.shard_map(
        local,
        mesh=mesh,
        in_specs=(
            P(("dom", "sub"), None, None),
            P(("dom", "sub"), None),
            P(("dom", "sub")),
            P(("dom", "sub"), None),
            P(("dom", "sub"), None),
            P(None, ("dom", "sub")),
            P(("dom", "sub")),
            P("dom", None),
            P("dom"),
        ),
        out_specs=P(("dom", "sub"), None, None),
        check_vma=False,
    )
```

```python
import functools
import math

import jax
import jax.numpy as jnp
from jax import lax
from jax.experimental import pallas as pl
from jax.experimental.pallas import tpu as pltpu
from jax.sharding import PartitionSpec as P

CUR_BIN = 2
SOFTEN_SQ = 0.04
LANES = 128
SCALE = math.sqrt(math.log2(math.e) / 4)
KAPPA = 0.5033782057491644
LEAD = 1.0644227815066034
POLY = (
    0.0006822818085192818,
    0.6891780368303475,
    -0.07494018001023989,
    -0.03418881002810906,
    0.008589076872810486,
)
MASS_SCALE = LEAD * SCALE / math.sqrt(math.pi)
MESH = pl.DeviceIdType.MESH
TILE = 144
PAIR = 3


def bf16_pieces(value):
    pieces = []
    for _ in range(3):
        mantissa, exponent = math.frexp(value)
        piece = math.ldexp(round(mantissa * 256), exponent - 8)
        pieces.append(piece)
        value -= piece
    return tuple(pieces)


SOFT = bf16_pieces(SOFTEN_SQ * SCALE * SCALE)


def split(value):
    high = value.astype(jnp.bfloat16).astype(jnp.float32)
    rest = value - high
    middle = rest.astype(jnp.bfloat16).astype(jnp.float32)
    return value, rest, rest - middle


def share_kernel(
    node_pos, node_mass, bins, homes, targets, target_groups, all_pos, all_mass, ranks, meta,
    send_sem, recv_sem, groups, share, stride,
):
    sharers = lax.axis_size("sub")
    domain, place = lax.axis_index("dom"), lax.axis_index("sub")
    barrier = pltpu.get_barrier_semaphore()
    others = [lax.rem(place + k, sharers) for k in range(1, sharers)]
    for other in others:
        pl.semaphore_signal(barrier, inc=1, device_id={"sub": other}, device_id_type=MESH)
    pl.semaphore_wait(barrier, sharers - 1)
    copies = []
    for k, other in enumerate(others):
        for j, (own, out) in enumerate(((node_pos, all_pos), (node_mass, all_mass))):
            copy = pltpu.make_async_remote_copy(
                src_ref=own,
                dst_ref=out.at[place],
                send_sem=send_sem.at[j, k],
                recv_sem=recv_sem.at[j, k],
                device_id={"sub": other},
                device_id_type=MESH,
            )
            copy.start()
            copies.append(copy)
    all_pos[place] = node_pos[...]
    all_mass[place] = node_mass[...]

    blocks, width = bins.shape
    most = targets.shape[0]
    active = bins[...] <= CUR_BIN
    flags = jnp.where(active, 1.0, 0.0).astype(jnp.bfloat16)
    upper = lax.broadcasted_iota(jnp.int32, (width, width), 0) <= lax.broadcasted_iota(
        jnp.int32, (width, width), 1
    )
    running = jnp.dot(
        flags,
        jnp.where(upper, 1.0, 0.0).astype(jnp.bfloat16),
        preferred_element_type=jnp.float32,
    ).astype(jnp.int32)
    ranks[...] = jnp.where(active, running - 1, -1)
    number = lax.dot_general(
        jnp.ones((8, width), jnp.bfloat16),
        flags,
        (((1,), (1,)), ((), ())),
        preferred_element_type=jnp.float32,
    ).astype(jnp.int32)
    holders = groups // share

    def places(owner, group):
        slot = owner * holders + lax.div(group, share)
        inner = lax.rem(group, share)
        return slot * LANES + inner, slot * stride + inner * 8

    key, line = places(domain, homes[...])
    meta[0:1] = key
    meta[most + 1 : most + 2] = line
    key, line = places(jnp.maximum(targets[...], 0), target_groups[...])
    meta[1 : most + 1] = jnp.where(targets[...] >= 0, key, LANES - 1)
    meta[most + 2 : 2 * most + 2] = line
    meta[2 * most + 2 : 2 * most + 3] = number[0:1]
    for copy in copies:
        copy.wait()


def gather_kernel(all_pos, all_mass, lists, list_counts, out, stack):
    sharers, _, per_device = all_pos.shape
    height = per_device // LANES
    total, length = lists.shape
    share = total // sharers
    place = lax.axis_index("sub")
    f32, bf16 = jnp.float32, jnp.bfloat16
    for owner in range(sharers):
        for high in range(height):
            at = (owner * height + high) * 4
            stack[at : at + 3] = all_pos[owner, :, high * LANES : (high + 1) * LANES] * SCALE
            stack[at + 3 : at + 4] = all_mass[owner, high : high + 1, :] * MASS_SCALE
    half = sharers * height // 2
    rows = half * 4
    pieces = [
        piece.astype(bf16)
        for piece in split(jnp.concatenate([stack[0:rows], stack[rows : 2 * rows]], axis=1))
    ]
    order = lax.broadcasted_iota(jnp.int32, (2 * LANES, length), 0)
    pair = lax.broadcasted_iota(jnp.int32, (8, length), 0) >> 2
    lane = lax.broadcasted_iota(jnp.int32, (4, length), 1)
    axis = lax.broadcasted_iota(jnp.int32, (4, length), 0)

    def one(local):
        group = place * share + local
        index = lists[pl.ds(group, 1), :]
        high = index >> 7
        far = jnp.where(high >= half, 1, 0)
        low = (index & (LANES - 1)) + far * LANES
        high = jnp.broadcast_to(high - far * half, (8, length)) - pair
        pick = jnp.where(order == low, 1.0, 0.0).astype(bf16)
        found = sum(jnp.dot(piece, pick, preferred_element_type=f32) for piece in pieces)
        total = jnp.zeros((8, length), f32)
        for t in range(rows // 8):
            total = jnp.where(high == 2 * t, found[8 * t : 8 * t + 8], total)
        picked = total[0:4] + total[4:8]
        valid = (axis < 3) | (lane < list_counts[group])
        picked = jnp.where(valid, picked, 0.0)
        out[pl.ds(pl.multiple_of(local * 8, 8), 8), :] = jnp.concatenate(
            [picked[:, 0:LANES], picked[:, LANES : 2 * LANES]], axis=0
        )

    def some(step, carry):
        for k in range(2):
            one(step * 2 + k)
        return carry

    lax.fori_loop(0, share // 2, some, 0)
    lane8 = lax.broadcasted_iota(jnp.int32, (8, LANES), 1)
    tail = jnp.zeros((8, LANES), jnp.int32)
    for local in range(share):
        tail = jnp.where(lane8 == local, list_counts[place * share + local], tail)
    out[share * 8 : share * 8 + 8, :] = tail.astype(f32)


def exchange_kernel(
    own, out, counts, z_send, z_recv, p_send, p_recv, q_send, q_recv, n_send, n_recv
):
    sharers, domains = lax.axis_size("sub"), lax.axis_size("dom")
    domain, place = lax.axis_index("dom"), lax.axis_index("sub")
    deep, wide = domains // 2, sharers // 2
    core = lax.rem(place, 2)
    across = place // 2
    layer, side = domain // 2, lax.rem(domain, 2)
    sibling = {"sub": place + 1 - 2 * core}
    barrier = pltpu.get_barrier_semaphore()

    def shifted(at, by, size):
        return lax.rem(at + by + size, size)

    def device(dz, dy, dx):
        return {
            "dom": shifted(layer, dz, deep) * 2 + shifted(side, dy, 2),
            "sub": shifted(across, dx, wide) * 2 + core,
        }

    def slot(dz, dy, dx):
        there = device(-dz, -dy, -dx)
        return there["dom"] * sharers + there["sub"]

    peers = [device(k, 0, 0) for k in range(1, deep)]
    peers += [device(0, 1, 0)] + [device(0, 0, k) for k in range(1, wide)] + [sibling]
    for peer in peers:
        pl.semaphore_signal(barrier, inc=1, device_id=peer, device_id_type=MESH)
    pl.semaphore_wait(barrier, len(peers))

    def run(side_first):
        first, second = (2, wide) if side_first else (wide, 2)

        def cell(k, j, i):
            return (k, j, i) if side_first else (k, i, j)

        def block(k, j, i):
            return own if (k, j, i) == (0, 0, 0) else out.at[slot(*cell(k, j, i))]

        def copy(source, at, send, recv, there):
            return pltpu.make_async_remote_copy(
                src_ref=source,
                dst_ref=out.at[at],
                send_sem=send,
                recv_sem=recv,
                device_id=there,
                device_id_type=MESH,
            )

        def z_copy(k):
            return copy(own, slot(0, 0, 0), z_send.at[k], z_recv.at[k], device(k, 0, 0))

        def p_copy(k, j):
            at = slot(*cell(k, 0, 0))
            return copy(
                block(k, 0, 0), at, p_send.at[k, j], p_recv.at[k, j], device(*cell(0, j, 0))
            )

        def q_copy(k, j, i):
            at = slot(*cell(k, j, 0))
            return copy(
                block(k, j, 0), at, q_send.at[k, j, i], q_recv.at[k, j, i], device(*cell(0, 0, i))
            )

        def n_copy(k, j, i):
            c = cell(k, j, i)
            return copy(block(k, j, i), slot(*c), n_send.at[c], n_recv.at[c], sibling)

        started = []

        def start(item):
            item.start()
            started.append(item)

        def after_z(k):
            for j in range(1, first):
                start(p_copy(k, j))
            for i in range(1, second):
                start(q_copy(k, 0, i))
            start(n_copy(k, 0, 0))

        def after_p(k, j):
            for i in range(1, second):
                start(q_copy(k, j, i))
            start(n_copy(k, j, 0))

        def take_p(k):
            for j in range(1, first):
                p_copy(k, j).wait_recv()
                after_p(k, j)

        for k in range(1, deep):
            start(z_copy(k))
        after_z(0)
        out[slot(0, 0, 0)] = own[...]
        take_p(0)
        for k in range(1, deep):
            z_copy(k).wait_recv()
            after_z(k)
            if k > 1:
                take_p(k - 1)
        take_p(deep - 1)
        for k in range(deep):
            for j in range(first):
                for i in range(1, second):
                    q_copy(k, j, i).wait_recv()
                    start(n_copy(k, j, i))
        for k in range(deep):
            for j in range(first):
                for i in range(second):
                    n_copy(k, j, i).wait_recv()
        for item in started:
            item.wait_send()

    pl.when(core == 0)(lambda: run(True))
    pl.when(core == 1)(lambda: run(False))
    tail = out.shape[1] - 8
    counts[...] = out[:, tail, :].astype(jnp.int32)


def radial(range_sq):
    near = lax.rsqrt(range_sq)
    fall = 1.0 / (range_sq * jnp.exp2(range_sq))
    z = 1.0 / (near + KAPPA)
    poly = z * POLY[-1] + POLY[-2]
    for coefficient in POLY[-3::-1]:
        poly = poly * z + coefficient
    return (poly + near) * fall


def pull_kernel(
    meta, counts, pos, ranks, table, out,
    items, beyond, sinks, totals, later_range, later_weight, later_nodes, last_nodes,
):
    blocks = meta.shape[1]
    visits = (meta.shape[0] - 1) // 2
    width = pos.shape[2]
    tiles = sinks.shape[0] // blocks
    spare = tiles * blocks
    f32, bf16 = jnp.float32, jnp.bfloat16
    sub8 = lax.broadcasted_iota(jnp.int32, (8, width), 0)
    axis8 = sub8 & 3
    by_rows = (((1,), (1,)), ((), ()))
    order = lax.broadcasted_iota(jnp.int32, (TILE, width), 0)
    lane48 = lax.broadcasted_iota(jnp.int32, (TILE, 48), 1)
    soft_high, soft_rest, soft_last = SOFT
    soft = jnp.where(
        lane48 == 11,
        soft_high,
        jnp.where(lane48 == 27, soft_rest, jnp.where(lane48 == 43, soft_last, 0.0)),
    )

    def axes(first, second, third, fourth, at):
        return jnp.where(at == 0, first, jnp.where(at == 1, second, jnp.where(at == 2, third, fourth)))

    def prepare(block, tile):
        line = [
            jnp.broadcast_to(pos[axis, pl.ds(block, 1), :] * SCALE, (8, width))
            for axis in range(3)
        ]
        norm = line[0] * line[0] + line[1] * line[1] + line[2] * line[2]
        pieces = split(axes(line[0], line[1], line[2], 0.0, axis8) * -2.0)
        norms = split(norm)
        parts = []
        for k in range(3):
            tail = jnp.where(sub8 == 7, norms[k], 1.0 if k == 0 else 0.0)
            parts.append(pieces[k])
            parts.append(jnp.where(sub8 < 3, pieces[k], jnp.where(sub8 == 3, 0.0, tail)))
        wide = jnp.concatenate(parts, axis=0).astype(bf16)
        rank = ranks[pl.ds(block, 1), :]

        at = tile * blocks + block
        pick = jnp.where(order == rank - tile * TILE, 1.0, 0.0).astype(bf16)
        held = lax.dot_general(pick, wide, by_rows, preferred_element_type=f32)
        sinks[at] = (held + soft).astype(bf16)
        totals[at] = jnp.zeros((TILE, LANES), f32)

    def list_items(tile, block, at):
        for visit in range(visits):
            key = meta[visit, block]
            count = counts[key >> 7, key & (LANES - 1)]
            code = meta[visits + visit, block] + (tile * blocks + block) * 65536
            items[at] = code
            at = at + jnp.minimum(count, 1)
            items[at] = code + 4
            at = at + jnp.where(count > LANES, 1, 0)
        return at

    def first(step, carry):
        at, extra = carry
        for k in range(4):
            block = step * 4 + k
            prepare(block, 0)
            at = list_items(0, block, at)
            for tile in range(1, tiles):
                beyond[extra] = block + tile * blocks
                extra = extra + jnp.where(meta[2 * visits, block] > tile * TILE, 1, 0)
        return at, extra

    def more(step, at):
        block = lax.rem(beyond[step], blocks)
        tile = beyond[step] // blocks
        prepare(block, tile)
        return list_items(tile, block, at)

    sinks[spare] = soft.astype(bf16)
    totals[spare] = jnp.zeros((TILE, LANES), f32)
    number, extra = lax.fori_loop(0, blocks // 4, first, (jnp.int32(0), jnp.int32(0)))
    number = lax.fori_loop(0, extra, more, number)
    for k in range(8 * PAIR):
        items[number + k] = spare * 65536

    sub = lax.broadcasted_iota(jnp.int32, (8, LANES), 0)
    axis = sub & 3

    def begin(item):
        code = items[item]
        line = code & 65535
        at = code >> 16
        row = [jnp.broadcast_to(table[pl.ds(line + f, 1), :], (8, LANES)) for f in range(4)]
        norm = row[0] * row[0] + row[1] * row[1] + row[2] * row[2]
        flat = axes(row[0], row[1], row[2], row[3], axis)
        pieces = split(flat)
        norms = split(norm)
        tail = jnp.where(
            sub == 4, norms[0], jnp.where(sub == 5, norms[1], jnp.where(sub == 6, norms[2], 1.0))
        )
        group = jnp.concatenate(
            [
                jnp.where(sub < 4, pieces[0], pieces[1]),
                jnp.where(sub < 3, pieces[2], tail),
            ],
            axis=0,
        ).astype(bf16)
        weighted = split(jnp.where(axis == 3, flat, flat * row[3]))
        moment = jnp.concatenate(
            [
                jnp.where(sub < 4, weighted[0], weighted[1]),
                jnp.where(sub < 4, weighted[2], 0.0),
            ],
            axis=0,
        ).astype(bf16)
        range_sq = jnp.dot(
            sinks[at], jnp.concatenate([group] * 3, axis=0), preferred_element_type=f32
        )
        return range_sq, jnp.concatenate([moment] * 2, axis=1)

    def weigh(range_sq):
        weight = radial(range_sq)
        high = weight.astype(bf16)
        low = (weight - high.astype(f32)).astype(bf16)
        return jnp.concatenate([high, low], axis=1)

    def gather(weight, moment):
        return lax.dot_general(weight, moment, by_rows, preferred_element_type=f32)

    def add(item, pull):
        at = items[item] >> 16
        totals[at, :, 0:16] += pull

    for k in range(2 * PAIR):
        later_range[k], later_nodes[k] = begin(k)
    for k in range(PAIR):
        later_weight[k] = jnp.zeros(later_weight.shape[1:], bf16)
        last_nodes[k] = jnp.zeros(last_nodes.shape[1:], bf16)

    def main(step, carry):
        base = step * (2 * PAIR)
        before = [gather(later_weight[k], last_nodes[k]) for k in range(PAIR)]
        after = [begin(base + 2 * PAIR + k) for k in range(2 * PAIR)]
        now = [gather(weigh(later_range[k]), later_nodes[k]) for k in range(PAIR)]
        for k in range(PAIR):
            add(jnp.where(step > 0, base - PAIR + k, number), before[k])
        for k in range(PAIR):
            later_weight[k] = weigh(later_range[PAIR + k])
            last_nodes[k] = later_nodes[PAIR + k]
        for k in range(PAIR):
            add(base + k, now[k])
        for k in range(2 * PAIR):
            later_range[k], later_nodes[k] = after[k]
        return carry

    groups = (number + PAIR - 1) // PAIR
    lax.fori_loop(0, groups // 2 + 1, main, 0)

    lane16 = lax.broadcasted_iota(jnp.int32, (TILE, LANES), 1)
    wide_tile = -(-TILE // LANES) * LANES

    def laid(flat, block, tile):
        flat = flat[0:4] + flat[4:8] + flat[8:12]
        flat = jnp.concatenate([flat, flat], axis=0)
        rank = jnp.broadcast_to(ranks[pl.ds(block, 1), :] - tile * TILE, (8, width))
        parts = []
        for k in range(0, width, LANES):
            at = rank[:, k : k + LANES]
            low = at & (LANES - 1)
            part = jnp.zeros((8, LANES), f32)
            for j in range(0, wide_tile, LANES):
                piece = jnp.take_along_axis(
                    flat[:, j : j + LANES], low, axis=1, mode="promise_in_bounds"
                )
                here = (at >= j) & (at < min(j + LANES, TILE))
                part = jnp.where(here, piece, part)
            parts.append(part)
        return jnp.concatenate(parts, axis=1)

    def turn(value):
        value = jnp.concatenate(
            [value, jnp.zeros((wide_tile - TILE, LANES), f32)], axis=0
        )
        return jnp.transpose(value)

    def store(block, sums):
        for axis in range(3):
            there = pos[axis, pl.ds(block, 1), :] * SCALE
            out[axis, pl.ds(block, 1), :] = sums[axis : axis + 1] - sums[3:4] * there

    def last(step, carry):
        packed = totals[step * 8]
        for k in range(1, 8):
            moved = pltpu.roll(totals[step * 8 + k], 16 * k, 1)
            packed = jnp.where(lane16 < 16 * k, packed, moved)
        turned = turn(packed)
        for k in range(8):
            store(step * 8 + k, laid(turned[16 * k : 16 * k + 16], step * 8 + k, 0))
        return carry

    lax.fori_loop(0, blocks // 8, last, 0)

    def rest(step, carry):
        block = lax.rem(beyond[step], blocks)
        sums = laid(turn(totals[beyond[step]])[0:16], block, beyond[step] // blocks)
        for axis in range(3):
            there = pos[axis, pl.ds(block, 1), :] * SCALE
            out[axis, pl.ds(block, 1), :] += sums[axis : axis + 1] - sums[3:4] * there
        return carry

    lax.fori_loop(0, extra, rest, 0)


def pull_call(meta, counts, pos, ranks, table, length):
    blocks, width = ranks.shape
    halves = length // LANES
    visits = (meta.shape[0] - 1) // 2
    tiles = -(-width // TILE)
    spare = tiles * blocks
    scratch = [
        pltpu.SMEM((blocks * visits * halves * tiles + 16 * PAIR,), jnp.int32),
        pltpu.SMEM((spare + 1,), jnp.int32),
        pltpu.VMEM((spare + 1, TILE, 48), jnp.bfloat16),
        pltpu.VMEM((spare + 1, TILE, LANES), jnp.float32),
        pltpu.VMEM((2 * PAIR, TILE, LANES), jnp.float32),
        pltpu.VMEM((PAIR, TILE, 2 * LANES), jnp.bfloat16),
        pltpu.VMEM((2 * PAIR, 16, 2 * LANES), jnp.bfloat16),
        pltpu.VMEM((PAIR, 16, 2 * LANES), jnp.bfloat16),
    ]
    smem = pl.BlockSpec(memory_space=pltpu.SMEM)
    vmem = pl.BlockSpec(memory_space=pltpu.VMEM)
    return pl.pallas_call(
        pull_kernel,
        out_shape=jax.ShapeDtypeStruct((3, blocks, width), jnp.float32),
        in_specs=[smem] * 2 + [vmem] * 3,
        out_specs=vmem,
        scratch_shapes=scratch,
        compiler_params=pltpu.CompilerParams(vmem_limit_bytes=60 * 1024 * 1024),
    )(meta, counts, pos, ranks, table)


def local(
    positions,
    time_bins,
    home_groups,
    targets,
    target_groups,
    node_pos,
    node_mass,
    node_lists,
    list_counts,
):
    domains = lax.axis_size("dom")
    sharers = lax.axis_size("sub")
    devices = domains * sharers
    blocks, most = targets.shape
    width = positions.shape[2]
    groups, length = node_lists.shape
    share = groups // sharers
    stride = share * 8 + 8
    per_device = node_mass.shape[0]
    height = per_device // LANES
    f32, i32 = jnp.float32, jnp.int32
    vmem = pl.BlockSpec(memory_space=pltpu.VMEM)
    smem = pl.BlockSpec(memory_space=pltpu.SMEM)
    dma = pltpu.SemaphoreType.DMA

    all_pos, all_mass, ranks, meta = pl.pallas_call(
        functools.partial(share_kernel, groups=groups, share=share, stride=stride),
        out_shape=[
            jax.ShapeDtypeStruct((sharers, 3, per_device), f32),
            jax.ShapeDtypeStruct((sharers, height, LANES), f32),
            jax.ShapeDtypeStruct((blocks, width), i32),
            jax.ShapeDtypeStruct((2 * most + 3, blocks), i32),
        ],
        in_specs=[vmem] * 6,
        out_specs=[vmem] * 4,
        scratch_shapes=[dma((2, sharers - 1))] * 2,
        compiler_params=pltpu.CompilerParams(collective_id=0, has_side_effects=True),
    )(
        node_pos,
        node_mass.reshape(height, LANES),
        time_bins,
        home_groups.reshape(1, blocks),
        targets.T,
        target_groups.T,
    )
    sent = pl.pallas_call(
        gather_kernel,
        out_shape=jax.ShapeDtypeStruct((stride, LANES), f32),
        in_specs=[vmem] * 3 + [smem],
        out_specs=vmem,
        scratch_shapes=[pltpu.VMEM((sharers * height * 4, LANES), f32)],
    )(all_pos, all_mass, node_lists, list_counts)
    deep, wide = domains // 2, sharers // 2
    most_first = max(2, wide)
    table, counts = pl.pallas_call(
        exchange_kernel,
        out_shape=[
            jax.ShapeDtypeStruct((devices, stride, LANES), f32),
            jax.ShapeDtypeStruct((devices, LANES), i32),
        ],
        in_specs=[vmem],
        out_specs=[vmem] * 2,
        scratch_shapes=[dma((deep,))] * 2
        + [dma((deep, most_first))] * 2
        + [dma((deep, most_first, most_first))] * 2
        + [dma((deep, 2, wide))] * 2,
        compiler_params=pltpu.CompilerParams(
            collective_id=1, has_side_effects=True, vmem_limit_bytes=48 * 1024 * 1024
        ),
    )(sent)
    forces = pull_call(
        meta,
        counts,
        jnp.transpose(positions, (1, 0, 2)),
        ranks,
        table.reshape(-1, LANES),
        length,
    )
    return jnp.transpose(forces, (1, 0, 2))


def solution(mesh):
    return jax.shard_map(
        local,
        mesh=mesh,
        in_specs=(
            P(("dom", "sub"), None, None),
            P(("dom", "sub"), None),
            P(("dom", "sub")),
            P(("dom", "sub"), None),
            P(("dom", "sub"), None),
            P(None, ("dom", "sub")),
            P(("dom", "sub")),
            P("dom", None),
            P("dom"),
        ),
        out_specs=P(("dom", "sub"), None, None),
        check_vma=False,
    )
```

```python
import functools
import math

import jax
import jax.numpy as jnp
from jax import lax
from jax.experimental import pallas as pl
from jax.experimental.pallas import tpu as pltpu
from jax.sharding import PartitionSpec as P

CUR_BIN = 2
SOFTEN_SQ = 0.04
LANES = 128
SCALE = math.sqrt(math.log2(math.e) / 4)
KAPPA = 0.5033782057491644
LEAD = 1.0644227815066034
POLY = (
    0.0006822818085192818,
    0.6891780368303475,
    -0.07494018001023989,
    -0.03418881002810906,
    0.008589076872810486,
)
MASS_SCALE = LEAD * SCALE / math.sqrt(math.pi)
MESH = pl.DeviceIdType.MESH
TILE = 144
PAIR = 3


def bf16_pieces(value):
    pieces = []
    for _ in range(3):
        mantissa, exponent = math.frexp(value)
        piece = math.ldexp(round(mantissa * 256), exponent - 8)
        pieces.append(piece)
        value -= piece
    return tuple(pieces)


SOFT = bf16_pieces(SOFTEN_SQ * SCALE * SCALE)


def split(value):
    high = value.astype(jnp.bfloat16).astype(jnp.float32)
    rest = value - high
    middle = rest.astype(jnp.bfloat16).astype(jnp.float32)
    return value, rest, rest - middle


def fill_tables(bins, homes, targets, target_groups, ranks, meta, groups, share, stride):
    domain = lax.axis_index("dom")
    blocks, width = bins.shape
    most = targets.shape[0]
    active = bins[...] <= CUR_BIN
    flags = jnp.where(active, 1.0, 0.0).astype(jnp.bfloat16)
    upper = lax.broadcasted_iota(jnp.int32, (width, width), 0) <= lax.broadcasted_iota(
        jnp.int32, (width, width), 1
    )
    running = jnp.dot(
        flags,
        jnp.where(upper, 1.0, 0.0).astype(jnp.bfloat16),
        preferred_element_type=jnp.float32,
    ).astype(jnp.int32)
    ranks[...] = jnp.where(active, running - 1, -1)
    number = lax.dot_general(
        jnp.ones((8, width), jnp.bfloat16),
        flags,
        (((1,), (1,)), ((), ())),
        preferred_element_type=jnp.float32,
    ).astype(jnp.int32)
    holders = groups // share

    def places(owner, group):
        slot = owner * holders + lax.div(group, share)
        inner = lax.rem(group, share)
        return slot * LANES + inner, slot * stride + inner * 8

    key, line = places(domain, homes[...])
    meta[0:1] = key
    meta[most + 1 : most + 2] = line
    key, line = places(jnp.maximum(targets[...], 0), target_groups[...])
    meta[1 : most + 1] = jnp.where(targets[...] >= 0, key, LANES - 1)
    meta[most + 2 : 2 * most + 2] = line
    meta[2 * most + 2 : 2 * most + 3] = number[0:1]


def gather_lists(all_pos, all_mass, lists, list_counts, out, stack):
    sharers, _, per_device = all_pos.shape
    height = per_device // LANES
    total, length = lists.shape
    share = total // sharers
    place = lax.axis_index("sub")
    f32, bf16 = jnp.float32, jnp.bfloat16
    for owner in range(sharers):
        for high in range(height):
            at = (owner * height + high) * 4
            stack[at : at + 3] = all_pos[owner, :, high * LANES : (high + 1) * LANES] * SCALE
            stack[at + 3 : at + 4] = all_mass[owner, high : high + 1, :] * MASS_SCALE
    half = sharers * height // 2
    rows = half * 4
    pieces = [
        piece.astype(bf16)
        for piece in split(jnp.concatenate([stack[0:rows], stack[rows : 2 * rows]], axis=1))
    ]
    order = lax.broadcasted_iota(jnp.int32, (2 * LANES, length), 0)
    pair = lax.broadcasted_iota(jnp.int32, (8, length), 0) >> 2
    lane = lax.broadcasted_iota(jnp.int32, (4, length), 1)
    axis = lax.broadcasted_iota(jnp.int32, (4, length), 0)

    def one(local):
        group = place * share + local
        index = lists[pl.ds(group, 1), :]
        high = index >> 7
        far = jnp.where(high >= half, 1, 0)
        low = (index & (LANES - 1)) + far * LANES
        high = jnp.broadcast_to(high - far * half, (8, length)) - pair
        pick = jnp.where(order == low, 1.0, 0.0).astype(bf16)
        found = sum(jnp.dot(piece, pick, preferred_element_type=f32) for piece in pieces)
        total = jnp.zeros((8, length), f32)
        for t in range(rows // 8):
            total = jnp.where(high == 2 * t, found[8 * t : 8 * t + 8], total)
        picked = total[0:4] + total[4:8]
        valid = (axis < 3) | (lane < list_counts[group])
        picked = jnp.where(valid, picked, 0.0)
        out[pl.ds(pl.multiple_of(local * 8, 8), 8), :] = jnp.concatenate(
            [picked[:, 0:LANES], picked[:, LANES : 2 * LANES]], axis=0
        )

    def some(step, carry):
        for k in range(2):
            one(step * 2 + k)
        return carry

    lax.fori_loop(0, share // 2, some, 0)
    lane8 = lax.broadcasted_iota(jnp.int32, (8, LANES), 1)
    tail = jnp.zeros((8, LANES), jnp.int32)
    for local in range(share):
        tail = jnp.where(lane8 == local, list_counts[place * share + local], tail)
    out[share * 8 : share * 8 + 8, :] = tail.astype(f32)


def domain_kernel(
    node_pos, node_mass, bins, homes, targets, target_groups, lists, positions, list_counts,
    out, counts, ranks, meta, pos,
    own_pos, own_mass, own_bins, own_homes, own_targets, own_groups, own_lists,
    all_pos, all_mass, stack, own, own_counts,
    load_sem, s_send, s_recv, z_send, z_recv, f_send, p_send, p_recv, q_send, q_recv,
    n_send, n_recv, groups, share, stride,
):
    sharers, domains = lax.axis_size("sub"), lax.axis_size("dom")
    domain, place = lax.axis_index("dom"), lax.axis_index("sub")
    deep, wide = domains // 2, sharers // 2
    half = deep // 2
    core = lax.rem(place, 2)
    across = place // 2
    layer, side = domain // 2, lax.rem(domain, 2)
    upper = layer // half
    gate = (1 - upper) * half + upper * (half - 1)
    other_gate = (1 - upper) * (half - 1) + upper * half
    sibling = {"sub": place + 1 - 2 * core}
    barrier = pltpu.get_barrier_semaphore()

    def shifted(at, by, size):
        return lax.rem(at + by + size, size)

    def device(z, dy, dx):
        return {
            "dom": z * 2 + shifted(side, dy, 2),
            "sub": shifted(across, dx, wide) * 2 + core,
        }

    def slot(z, dy, dx):
        there = device(z, -dy, -dx)
        return there["dom"] * sharers + there["sub"]

    others = [{"sub": lax.rem(place + k, sharers)} for k in range(1, sharers)]
    peers = [device(shifted(layer, k, deep), 0, 0) for k in range(1, deep)]
    peers += [device(layer, 1, 0)] + others
    for peer in peers:
        pl.semaphore_signal(barrier, inc=1, device_id=peer, device_id_type=MESH)
    loads = [
        pltpu.make_async_copy(source, target, load_sem.at[k])
        for k, (source, target) in enumerate(
            (
                (node_pos, own_pos),
                (node_mass, own_mass),
                (bins, own_bins),
                (homes, own_homes),
                (targets, own_targets),
                (target_groups, own_groups),
                (lists, own_lists),
                (positions, pos),
                (list_counts, own_counts),
            )
        )
    ]
    for load in loads:
        load.start()
    for load in loads[:2]:
        load.wait()
    pl.semaphore_wait(barrier, len(peers))
    copies = []
    for k, other in enumerate(others):
        for j, (source, target) in enumerate(((own_pos, all_pos), (own_mass, all_mass))):
            share_copy = pltpu.make_async_remote_copy(
                src_ref=source,
                dst_ref=target.at[place],
                send_sem=s_send.at[j, k],
                recv_sem=s_recv.at[j, k],
                device_id=other,
                device_id_type=MESH,
            )
            share_copy.start()
            copies.append(share_copy)
    all_pos[place] = own_pos[...]
    all_mass[place] = own_mass[...]
    for load in loads[2:]:
        load.wait()
    for share_copy in copies:
        share_copy.wait_recv()
    gather_lists(all_pos, all_mass, own_lists, own_counts, own, stack)
    fill_tables(
        own_bins, own_homes, own_targets, own_groups, ranks, meta, groups, share, stride
    )

    def run(side_first):
        first, second = (2, wide) if side_first else (wide, 2)

        def cell(j, i):
            return (j, i) if side_first else (i, j)

        def copy(source, at, send, recv, there):
            return pltpu.make_async_remote_copy(
                src_ref=source,
                dst_ref=out.at[at],
                send_sem=send,
                recv_sem=recv,
                device_id=there,
                device_id_type=MESH,
            )

        mine = slot(layer, 0, 0)

        def z_copy(k, to):
            return copy(own, mine, z_send.at[k], z_recv.at[layer], device(to, 0, 0))

        def z_wait(z):
            copy(own, slot(z, 0, 0), z_send.at[0], z_recv.at[z], device(z, 0, 0)).wait_recv()

        def f_copy(z, k):
            to = upper * half + lax.rem(layer - upper * half + k, half)
            at = slot(z, 0, 0)
            return copy(
                out.at[at], at, f_send.at[lax.rem(z, half), k], z_recv.at[z], device(to, 0, 0)
            )

        def p_copy(z, j, source=None):
            at = slot(z, 0, 0)
            return copy(
                out.at[at] if source is None else source,
                at,
                p_send.at[z, j],
                p_recv.at[z, j],
                device(layer, *cell(j, 0)),
            )

        def q_copy(z, j, i, source=None):
            at = slot(z, *cell(j, 0))
            return copy(
                out.at[at] if source is None else source,
                at,
                q_send.at[z, j, i],
                q_recv.at[z, j, i],
                device(layer, *cell(0, i)),
            )

        def n_copy(z, j, i, source=None):
            c = cell(j, i)
            at = slot(z, *c)
            return copy(
                out.at[at] if source is None else source,
                at,
                n_send.at[(z,) + c],
                n_recv.at[(z,) + c],
                sibling,
            )

        def after_z(z, source=None):
            for j in range(1, first):
                p_copy(z, j, source).start()
            for i in range(1, second):
                q_copy(z, 0, i, source).start()
            n_copy(z, 0, 0, source).start()

        def take_z(z):
            z_wait(z)

            @pl.when((layer == other_gate) & (z // half != upper))
            def _():
                for k in range(1, half):
                    f_copy(z, k).start()

            after_z(z)

        def take_p(z):
            for j in range(1, first):
                p_copy(z, j).wait_recv()
                for i in range(1, second):
                    q_copy(z, j, i).start()
                n_copy(z, j, 0).start()

        def take_q(z):
            for j in range(first):
                for i in range(1, second):
                    q_copy(z, j, i).wait_recv()
                    n_copy(z, j, i).start()

        def at_distance(k, action):
            pl.when(layer + k < deep)(lambda: action(layer + k))
            pl.when(layer - k >= 0)(lambda: action(layer - k))

        for k in range(1, half):
            z_copy(k, upper * half + lax.rem(layer - upper * half + k, half)).start()
        z_copy(0, gate).start()
        after_z(layer, own)
        out[mine] = own[...]
        take_p(layer)
        for k in range(1, deep):
            at_distance(k, take_z)
            if k > 1:
                at_distance(k - 1, take_p)
        at_distance(deep - 1, take_p)
        take_q(layer)
        for k in range(1, deep):
            at_distance(k, take_q)
        for k in range(half):
            z_copy(k, gate).wait_send()

        @pl.when(layer == other_gate)
        def _():
            for z in range(half):
                for k in range(1, half):
                    f_copy(z, k).wait_send()

        for z in range(deep):
            for j in range(first):
                for i in range(second):
                    if i == 0 and j > 0:
                        p_copy(z, j).wait_send()
                    if i > 0:
                        q_copy(z, j, i).wait_send()
                    n_copy(z, j, i).wait()

    pl.when(core == 0)(lambda: run(True))
    pl.when(core == 1)(lambda: run(False))
    for share_copy in copies:
        share_copy.wait_send()
    tail = out.shape[1] - 8
    counts[...] = out[:, tail, :].astype(jnp.int32)


def radial(range_sq):
    near = lax.rsqrt(range_sq)
    fall = 1.0 / (range_sq * jnp.exp2(range_sq))
    z = 1.0 / (near + KAPPA)
    poly = z * POLY[-1] + POLY[-2]
    for coefficient in POLY[-3::-1]:
        poly = poly * z + coefficient
    return (poly + near) * fall


def pull_kernel(
    meta, counts, pos, ranks, table, out,
    items, beyond, sinks, totals, later_range, later_weight, later_nodes, last_nodes,
):
    blocks = meta.shape[1]
    visits = (meta.shape[0] - 1) // 2
    width = pos.shape[2]
    tiles = sinks.shape[0] // blocks
    spare = tiles * blocks
    f32, bf16 = jnp.float32, jnp.bfloat16
    sub8 = lax.broadcasted_iota(jnp.int32, (8, width), 0)
    axis8 = sub8 & 3
    by_rows = (((1,), (1,)), ((), ()))
    order = lax.broadcasted_iota(jnp.int32, (TILE, width), 0)
    lane48 = lax.broadcasted_iota(jnp.int32, (TILE, 48), 1)
    soft_high, soft_rest, soft_last = SOFT
    soft = jnp.where(
        lane48 == 11,
        soft_high,
        jnp.where(lane48 == 27, soft_rest, jnp.where(lane48 == 43, soft_last, 0.0)),
    )

    def axes(first, second, third, fourth, at):
        return jnp.where(at == 0, first, jnp.where(at == 1, second, jnp.where(at == 2, third, fourth)))

    def prepare(block, tile):
        line = [
            jnp.broadcast_to(pos[axis, pl.ds(block, 1), :] * SCALE, (8, width))
            for axis in range(3)
        ]
        norm = line[0] * line[0] + line[1] * line[1] + line[2] * line[2]
        pieces = split(axes(line[0], line[1], line[2], 0.0, axis8) * -2.0)
        norms = split(norm)
        parts = []
        for k in range(3):
            tail = jnp.where(sub8 == 7, norms[k], 1.0 if k == 0 else 0.0)
            parts.append(pieces[k])
            parts.append(jnp.where(sub8 < 3, pieces[k], jnp.where(sub8 == 3, 0.0, tail)))
        wide = jnp.concatenate(parts, axis=0).astype(bf16)
        rank = ranks[pl.ds(block, 1), :]

        at = tile * blocks + block
        pick = jnp.where(order == rank - tile * TILE, 1.0, 0.0).astype(bf16)
        held = lax.dot_general(pick, wide, by_rows, preferred_element_type=f32)
        sinks[at] = (held + soft).astype(bf16)
        totals[at] = jnp.zeros((TILE, LANES), f32)

    def list_items(tile, block, at):
        for visit in range(visits):
            key = meta[visit, block]
            count = counts[key >> 7, key & (LANES - 1)]
            code = meta[visits + visit, block] + (tile * blocks + block) * 65536
            items[at] = code
            at = at + jnp.minimum(count, 1)
            items[at] = code + 4
            at = at + jnp.where(count > LANES, 1, 0)
        return at

    def first(step, carry):
        at, extra = carry
        for k in range(4):
            block = step * 4 + k
            prepare(block, 0)
            at = list_items(0, block, at)
            for tile in range(1, tiles):
                beyond[extra] = block + tile * blocks
                extra = extra + jnp.where(meta[2 * visits, block] > tile * TILE, 1, 0)
        return at, extra

    def more(step, at):
        block = lax.rem(beyond[step], blocks)
        tile = beyond[step] // blocks
        prepare(block, tile)
        return list_items(tile, block, at)

    sinks[spare] = soft.astype(bf16)
    totals[spare] = jnp.zeros((TILE, LANES), f32)
    number, extra = lax.fori_loop(0, blocks // 4, first, (jnp.int32(0), jnp.int32(0)))
    number = lax.fori_loop(0, extra, more, number)
    for k in range(8 * PAIR):
        items[number + k] = spare * 65536

    sub = lax.broadcasted_iota(jnp.int32, (8, LANES), 0)
    axis = sub & 3

    def begin(item):
        code = items[item]
        line = code & 65535
        at = code >> 16
        row = [jnp.broadcast_to(table[pl.ds(line + f, 1), :], (8, LANES)) for f in range(4)]
        norm = row[0] * row[0] + row[1] * row[1] + row[2] * row[2]
        flat = axes(row[0], row[1], row[2], row[3], axis)
        pieces = split(flat)
        norms = split(norm)
        tail = jnp.where(
            sub == 4, norms[0], jnp.where(sub == 5, norms[1], jnp.where(sub == 6, norms[2], 1.0))
        )
        group = jnp.concatenate(
            [
                jnp.where(sub < 4, pieces[0], pieces[1]),
                jnp.where(sub < 3, pieces[2], tail),
            ],
            axis=0,
        ).astype(bf16)
        weighted = split(jnp.where(axis == 3, flat, flat * row[3]))
        moment = jnp.concatenate(
            [
                jnp.where(sub < 4, weighted[0], weighted[1]),
                jnp.where(sub < 4, weighted[2], 0.0),
            ],
            axis=0,
        ).astype(bf16)
        range_sq = jnp.dot(
            sinks[at], jnp.concatenate([group] * 3, axis=0), preferred_element_type=f32
        )
        return range_sq, jnp.concatenate([moment] * 2, axis=1)

    def weigh(range_sq):
        weight = radial(range_sq)
        high = weight.astype(bf16)
        low = (weight - high.astype(f32)).astype(bf16)
        return jnp.concatenate([high, low], axis=1)

    def gather(weight, moment):
        return lax.dot_general(weight, moment, by_rows, preferred_element_type=f32)

    def add(item, pull):
        at = items[item] >> 16
        totals[at, :, 0:16] += pull

    for k in range(2 * PAIR):
        later_range[k], later_nodes[k] = begin(k)
    for k in range(PAIR):
        later_weight[k] = jnp.zeros(later_weight.shape[1:], bf16)
        last_nodes[k] = jnp.zeros(last_nodes.shape[1:], bf16)

    def main(step, carry):
        base = step * (2 * PAIR)
        before = [gather(later_weight[k], last_nodes[k]) for k in range(PAIR)]
        after = [begin(base + 2 * PAIR + k) for k in range(2 * PAIR)]
        now = [gather(weigh(later_range[k]), later_nodes[k]) for k in range(PAIR)]
        for k in range(PAIR):
            add(jnp.where(step > 0, base - PAIR + k, number), before[k])
        for k in range(PAIR):
            later_weight[k] = weigh(later_range[PAIR + k])
            last_nodes[k] = later_nodes[PAIR + k]
        for k in range(PAIR):
            add(base + k, now[k])
        for k in range(2 * PAIR):
            later_range[k], later_nodes[k] = after[k]
        return carry

    groups = (number + PAIR - 1) // PAIR
    lax.fori_loop(0, groups // 2 + 1, main, 0)

    lane16 = lax.broadcasted_iota(jnp.int32, (TILE, LANES), 1)
    wide_tile = -(-TILE // LANES) * LANES

    def laid(flat, block, tile):
        flat = flat[0:4] + flat[4:8] + flat[8:12]
        flat = jnp.concatenate([flat, flat], axis=0)
        rank = jnp.broadcast_to(ranks[pl.ds(block, 1), :] - tile * TILE, (8, width))
        parts = []
        for k in range(0, width, LANES):
            at = rank[:, k : k + LANES]
            low = at & (LANES - 1)
            part = jnp.zeros((8, LANES), f32)
            for j in range(0, wide_tile, LANES):
                piece = jnp.take_along_axis(
                    flat[:, j : j + LANES], low, axis=1, mode="promise_in_bounds"
                )
                here = (at >= j) & (at < min(j + LANES, TILE))
                part = jnp.where(here, piece, part)
            parts.append(part)
        return jnp.concatenate(parts, axis=1)

    def turn(value):
        value = jnp.concatenate(
            [value, jnp.zeros((wide_tile - TILE, LANES), f32)], axis=0
        )
        return jnp.transpose(value)

    def store(block, sums):
        for axis in range(3):
            there = pos[axis, pl.ds(block, 1), :] * SCALE
            out[axis, pl.ds(block, 1), :] = sums[axis : axis + 1] - sums[3:4] * there

    def last(step, carry):
        packed = totals[step * 8]
        for k in range(1, 8):
            moved = pltpu.roll(totals[step * 8 + k], 16 * k, 1)
            packed = jnp.where(lane16 < 16 * k, packed, moved)
        turned = turn(packed)
        for k in range(8):
            store(step * 8 + k, laid(turned[16 * k : 16 * k + 16], step * 8 + k, 0))
        return carry

    lax.fori_loop(0, blocks // 8, last, 0)

    def rest(step, carry):
        block = lax.rem(beyond[step], blocks)
        sums = laid(turn(totals[beyond[step]])[0:16], block, beyond[step] // blocks)
        for axis in range(3):
            there = pos[axis, pl.ds(block, 1), :] * SCALE
            out[axis, pl.ds(block, 1), :] += sums[axis : axis + 1] - sums[3:4] * there
        return carry

    lax.fori_loop(0, extra, rest, 0)


def pull_call(meta, counts, pos, ranks, table, length):
    blocks, width = ranks.shape
    halves = length // LANES
    visits = (meta.shape[0] - 1) // 2
    tiles = -(-width // TILE)
    spare = tiles * blocks
    scratch = [
        pltpu.SMEM((blocks * visits * halves * tiles + 16 * PAIR,), jnp.int32),
        pltpu.SMEM((spare + 1,), jnp.int32),
        pltpu.VMEM((spare + 1, TILE, 48), jnp.bfloat16),
        pltpu.VMEM((spare + 1, TILE, LANES), jnp.float32),
        pltpu.VMEM((2 * PAIR, TILE, LANES), jnp.float32),
        pltpu.VMEM((PAIR, TILE, 2 * LANES), jnp.bfloat16),
        pltpu.VMEM((2 * PAIR, 16, 2 * LANES), jnp.bfloat16),
        pltpu.VMEM((PAIR, 16, 2 * LANES), jnp.bfloat16),
    ]
    smem = pl.BlockSpec(memory_space=pltpu.SMEM)
    vmem = pl.BlockSpec(memory_space=pltpu.VMEM)
    return pl.pallas_call(
        pull_kernel,
        out_shape=jax.ShapeDtypeStruct((3, blocks, width), jnp.float32),
        in_specs=[smem] * 2 + [vmem] * 3,
        out_specs=vmem,
        scratch_shapes=scratch,
        compiler_params=pltpu.CompilerParams(vmem_limit_bytes=36 * 1024 * 1024),
    )(meta, counts, pos, ranks, table)


def local(
    positions,
    time_bins,
    home_groups,
    targets,
    target_groups,
    node_pos,
    node_mass,
    node_lists,
    list_counts,
):
    domains = lax.axis_size("dom")
    sharers = lax.axis_size("sub")
    devices = domains * sharers
    blocks, most = targets.shape
    width = positions.shape[2]
    groups, length = node_lists.shape
    share = groups // sharers
    stride = share * 8 + 8
    per_device = node_mass.shape[0]
    height = per_device // LANES
    f32, i32 = jnp.float32, jnp.int32
    vmem = pl.BlockSpec(memory_space=pltpu.VMEM)
    dma = pltpu.SemaphoreType.DMA

    hbm = pl.BlockSpec(memory_space=pltpu.HBM)
    deep, wide = domains // 2, sharers // 2
    most_first = max(2, wide)
    table, counts, ranks, meta, pos = pl.pallas_call(
        functools.partial(domain_kernel, groups=groups, share=share, stride=stride),
        out_shape=[
            jax.ShapeDtypeStruct((devices, stride, LANES), f32),
            jax.ShapeDtypeStruct((devices, LANES), i32),
            jax.ShapeDtypeStruct((blocks, width), i32),
            jax.ShapeDtypeStruct((2 * most + 3, blocks), i32),
            jax.ShapeDtypeStruct((3, blocks, width), f32),
        ],
        in_specs=[hbm] * 9,
        out_specs=[vmem] * 5,
        scratch_shapes=[
            pltpu.VMEM((3, per_device), f32),
            pltpu.VMEM((height, LANES), f32),
            pltpu.VMEM((blocks, width), i32),
            pltpu.VMEM((1, blocks), i32),
            pltpu.VMEM((most, blocks), i32),
            pltpu.VMEM((most, blocks), i32),
            pltpu.VMEM((groups, length), i32),
            pltpu.VMEM((sharers, 3, per_device), f32),
            pltpu.VMEM((sharers, height, LANES), f32),
            pltpu.VMEM((sharers * height * 4, LANES), f32),
            pltpu.VMEM((stride, LANES), f32),
            pltpu.SMEM((groups,), i32),
            dma((9,)),
        ]
        + [dma((2, sharers - 1))] * 2
        + [dma((deep,))] * 2
        + [dma((deep, deep))]
        + [dma((deep, most_first))] * 2
        + [dma((deep, most_first, most_first))] * 2
        + [dma((deep, 2, wide))] * 2,
        compiler_params=pltpu.CompilerParams(
            collective_id=0, has_side_effects=True, vmem_limit_bytes=24 * 1024 * 1024
        ),
    )(
        *(
            pltpu.with_memory_space_constraint(array, pltpu.HBM)
            for array in (
                node_pos,
                node_mass.reshape(height, LANES),
                time_bins,
                home_groups.reshape(1, blocks),
                targets.T,
                target_groups.T,
                node_lists,
                jnp.transpose(positions, (1, 0, 2)),
                list_counts,
            )
        )
    )
    forces = pull_call(
        meta,
        counts,
        pos,
        ranks,
        table.reshape(-1, LANES),
        length,
    )
    return jnp.transpose(forces, (1, 0, 2))


def solution(mesh):
    return jax.shard_map(
        local,
        mesh=mesh,
        in_specs=(
            P(("dom", "sub"), None, None),
            P(("dom", "sub"), None),
            P(("dom", "sub")),
            P(("dom", "sub"), None),
            P(("dom", "sub"), None),
            P(None, ("dom", "sub")),
            P(("dom", "sub")),
            P("dom", None),
            P("dom"),
        ),
        out_specs=P(("dom", "sub"), None, None),
        check_vma=False,
    )
```

```python
import functools
import math

import jax
import jax.numpy as jnp
from jax import lax
from jax.experimental import pallas as pl
from jax.experimental.pallas import tpu as pltpu
from jax.sharding import PartitionSpec as P

CUR_BIN = 2
SOFTEN_SQ = 0.04
LANES = 128
SCALE = math.sqrt(math.log2(math.e) / 4)
KAPPA = 0.5033782057491644
LEAD = 1.0644227815066034
POLY = (
    0.0006822818085192818,
    0.6891780368303475,
    -0.07494018001023989,
    -0.03418881002810906,
    0.008589076872810486,
)
MASS_SCALE = LEAD * SCALE / math.sqrt(math.pi)
MESH = pl.DeviceIdType.MESH
TILE = 144
PAIR = 3


def bf16_pieces(value):
    pieces = []
    for _ in range(3):
        mantissa, exponent = math.frexp(value)
        piece = math.ldexp(round(mantissa * 256), exponent - 8)
        pieces.append(piece)
        value -= piece
    return tuple(pieces)


SOFT = bf16_pieces(SOFTEN_SQ * SCALE * SCALE)


def split(value):
    high = value.astype(jnp.bfloat16).astype(jnp.float32)
    rest = value - high
    middle = rest.astype(jnp.bfloat16).astype(jnp.float32)
    return value, rest, rest - middle


def fill_tables(bins, homes, targets, target_groups, ranks, meta, groups, share, stride):
    domain = lax.axis_index("dom")
    blocks, width = bins.shape
    most = targets.shape[0]
    active = bins[...] <= CUR_BIN
    flags = jnp.where(active, 1.0, 0.0).astype(jnp.bfloat16)
    upper = lax.broadcasted_iota(jnp.int32, (width, width), 0) <= lax.broadcasted_iota(
        jnp.int32, (width, width), 1
    )
    running = jnp.dot(
        flags,
        jnp.where(upper, 1.0, 0.0).astype(jnp.bfloat16),
        preferred_element_type=jnp.float32,
    ).astype(jnp.int32)
    ranks[...] = jnp.where(active, running - 1, -1)
    number = lax.dot_general(
        jnp.ones((8, width), jnp.bfloat16),
        flags,
        (((1,), (1,)), ((), ())),
        preferred_element_type=jnp.float32,
    ).astype(jnp.int32)
    holders = groups // share

    def places(owner, group):
        slot = owner * holders + lax.div(group, share)
        inner = lax.rem(group, share)
        return slot * LANES + inner, slot * stride + inner * 8

    key, line = places(domain, homes[...])
    meta[0:1] = key
    meta[most + 1 : most + 2] = line
    key, line = places(jnp.maximum(targets[...], 0), target_groups[...])
    meta[1 : most + 1] = jnp.where(targets[...] >= 0, key, LANES - 1)
    meta[most + 2 : 2 * most + 2] = line
    meta[2 * most + 2 : 2 * most + 3] = number[0:1]


def gather_lists(all_pos, all_mass, lists, list_counts, out, stack):
    sharers, _, per_device = all_pos.shape
    height = per_device // LANES
    total, length = lists.shape
    share = total // sharers
    place = lax.axis_index("sub")
    f32, bf16 = jnp.float32, jnp.bfloat16
    for owner in range(sharers):
        for high in range(height):
            at = (owner * height + high) * 4
            stack[at : at + 3] = all_pos[owner, :, high * LANES : (high + 1) * LANES] * SCALE
            stack[at + 3 : at + 4] = all_mass[owner, high : high + 1, :] * MASS_SCALE
    half = sharers * height // 2
    rows = half * 4
    pieces = [
        piece.astype(bf16)
        for piece in split(jnp.concatenate([stack[0:rows], stack[rows : 2 * rows]], axis=1))
    ]
    order = lax.broadcasted_iota(jnp.int32, (2 * LANES, length), 0)
    pair = lax.broadcasted_iota(jnp.int32, (8, length), 0) >> 2
    lane = lax.broadcasted_iota(jnp.int32, (4, length), 1)
    axis = lax.broadcasted_iota(jnp.int32, (4, length), 0)

    def one(local):
        group = place * share + local
        index = lists[pl.ds(group, 1), :]
        high = index >> 7
        far = jnp.where(high >= half, 1, 0)
        low = (index & (LANES - 1)) + far * LANES
        high = jnp.broadcast_to(high - far * half, (8, length)) - pair
        pick = jnp.where(order == low, 1.0, 0.0).astype(bf16)
        found = sum(jnp.dot(piece, pick, preferred_element_type=f32) for piece in pieces)
        total = jnp.zeros((8, length), f32)
        for t in range(rows // 8):
            total = jnp.where(high == 2 * t, found[8 * t : 8 * t + 8], total)
        picked = total[0:4] + total[4:8]
        valid = (axis < 3) | (lane < list_counts[group])
        picked = jnp.where(valid, picked, 0.0)
        out[pl.ds(pl.multiple_of(local * 8, 8), 8), :] = jnp.concatenate(
            [picked[:, 0:LANES], picked[:, LANES : 2 * LANES]], axis=0
        )

    def some(step, carry):
        for k in range(2):
            one(step * 2 + k)
        return carry

    lax.fori_loop(0, share // 2, some, 0)
    lane8 = lax.broadcasted_iota(jnp.int32, (8, LANES), 1)
    tail = jnp.zeros((8, LANES), jnp.int32)
    for local in range(share):
        tail = jnp.where(lane8 == local, list_counts[place * share + local], tail)
    out[share * 8 : share * 8 + 8, :] = tail.astype(f32)


def domain_kernel(
    node_pos, node_mass, bins, homes, targets, target_groups, lists, positions, list_counts,
    out, counts, ranks, meta, pos,
    own_pos, own_mass, own_bins, own_homes, own_targets, own_groups, own_lists,
    all_pos, all_mass, stack, own, own_counts,
    load_sem, s_send, s_recv, z_send, z_recv, f_send, p_send, p_recv, q_send, q_recv,
    n_send, n_recv, groups, share, stride,
):
    sharers, domains = lax.axis_size("sub"), lax.axis_size("dom")
    domain, place = lax.axis_index("dom"), lax.axis_index("sub")
    deep, wide = domains // 2, sharers // 2
    half = deep // 2
    core = lax.rem(place, 2)
    across = place // 2
    layer, side = domain // 2, lax.rem(domain, 2)
    upper = layer // half
    gate = (1 - upper) * half + upper * (half - 1)
    other_gate = (1 - upper) * (half - 1) + upper * half
    sibling = {"sub": place + 1 - 2 * core}
    barrier = pltpu.get_barrier_semaphore()

    def shifted(at, by, size):
        return lax.rem(at + by + size, size)

    def device(z, dy, dx):
        return {
            "dom": z * 2 + shifted(side, dy, 2),
            "sub": shifted(across, dx, wide) * 2 + core,
        }

    def slot(z, dy, dx):
        there = device(z, -dy, -dx)
        return there["dom"] * sharers + there["sub"]

    others = [{"sub": lax.rem(place + k, sharers)} for k in range(1, sharers)]
    peers = [device(shifted(layer, k, deep), 0, 0) for k in range(1, deep)]
    peers += [device(layer, 1, 0)] + others
    for peer in peers:
        pl.semaphore_signal(barrier, inc=1, device_id=peer, device_id_type=MESH)
    loads = [
        pltpu.make_async_copy(source, target, load_sem.at[k])
        for k, (source, target) in enumerate(
            (
                (node_pos, own_pos),
                (node_mass, own_mass),
                (bins, own_bins),
                (homes, own_homes),
                (targets, own_targets),
                (target_groups, own_groups),
                (lists, own_lists),
                (positions, pos),
                (list_counts, own_counts),
            )
        )
    ]
    for load in loads:
        load.start()
    for load in loads[:2]:
        load.wait()
    pl.semaphore_wait(barrier, len(peers))
    copies = []
    for k, other in enumerate(others):
        for j, (source, target) in enumerate(((own_pos, all_pos), (own_mass, all_mass))):
            share_copy = pltpu.make_async_remote_copy(
                src_ref=source,
                dst_ref=target.at[place],
                send_sem=s_send.at[j, k],
                recv_sem=s_recv.at[j, k],
                device_id=other,
                device_id_type=MESH,
            )
            share_copy.start()
            copies.append(share_copy)
    all_pos[place] = own_pos[...]
    all_mass[place] = own_mass[...]
    for load in loads[2:]:
        load.wait()
    for share_copy in copies:
        share_copy.wait_recv()
    gather_lists(all_pos, all_mass, own_lists, own_counts, own, stack)
    fill_tables(
        own_bins, own_homes, own_targets, own_groups, ranks, meta, groups, share, stride
    )

    def run(side_first):
        first, second = (2, wide) if side_first else (wide, 2)

        def cell(j, i):
            return (j, i) if side_first else (i, j)

        def copy(source, at, send, recv, there):
            return pltpu.make_async_remote_copy(
                src_ref=source,
                dst_ref=out.at[at],
                send_sem=send,
                recv_sem=recv,
                device_id=there,
                device_id_type=MESH,
            )

        mine = slot(layer, 0, 0)

        def z_copy(k, to):
            return copy(own, mine, z_send.at[k], z_recv.at[layer], device(to, 0, 0))

        def z_wait(z):
            copy(own, slot(z, 0, 0), z_send.at[0], z_recv.at[z], device(z, 0, 0)).wait_recv()

        def f_copy(z, k):
            to = upper * half + lax.rem(layer - upper * half + k, half)
            at = slot(z, 0, 0)
            return copy(
                out.at[at], at, f_send.at[lax.rem(z, half), k], z_recv.at[z], device(to, 0, 0)
            )

        def p_copy(z, j, source=None):
            at = slot(z, 0, 0)
            return copy(
                out.at[at] if source is None else source,
                at,
                p_send.at[z, j],
                p_recv.at[z, j],
                device(layer, *cell(j, 0)),
            )

        def q_copy(z, j, i, source=None):
            at = slot(z, *cell(j, 0))
            return copy(
                out.at[at] if source is None else source,
                at,
                q_send.at[z, j, i],
                q_recv.at[z, j, i],
                device(layer, *cell(0, i)),
            )

        def n_copy(z, j, i, source=None):
            c = cell(j, i)
            at = slot(z, *c)
            return copy(
                out.at[at] if source is None else source,
                at,
                n_send.at[(z,) + c],
                n_recv.at[(z,) + c],
                sibling,
            )

        def after_z(z, source=None):
            for j in range(1, first):
                p_copy(z, j, source).start()
            for i in range(1, second):
                q_copy(z, 0, i, source).start()
            n_copy(z, 0, 0, source).start()

        def take_z(z):
            z_wait(z)

            @pl.when((layer == other_gate) & (z // half != upper))
            def _():
                for k in range(1, half):
                    f_copy(z, k).start()

            after_z(z)

        def take_p(z):
            for j in range(1, first):
                p_copy(z, j).wait_recv()
                for i in range(1, second):
                    q_copy(z, j, i).start()
                n_copy(z, j, 0).start()

        def take_q(z):
            for j in range(first):
                for i in range(1, second):
                    q_copy(z, j, i).wait_recv()
                    n_copy(z, j, i).start()

        def at_distance(k, action):
            pl.when(layer + k < deep)(lambda: action(layer + k))
            pl.when(layer - k >= 0)(lambda: action(layer - k))

        for k in range(1, half):
            z_copy(k, upper * half + lax.rem(layer - upper * half + k, half)).start()
        z_copy(0, gate).start()
        after_z(layer, own)
        out[mine] = own[...]
        take_p(layer)
        for k in range(1, deep):
            at_distance(k, take_z)
            if k > 1:
                at_distance(k - 1, take_p)
        at_distance(deep - 1, take_p)
        take_q(layer)
        for k in range(1, deep):
            at_distance(k, take_q)
        for k in range(half):
            z_copy(k, gate).wait_send()

        @pl.when(layer == other_gate)
        def _():
            for z in range(half):
                for k in range(1, half):
                    f_copy(z, k).wait_send()

        for z in range(deep):
            for j in range(first):
                for i in range(second):
                    if i == 0 and j > 0:
                        p_copy(z, j).wait_send()
                    if i > 0:
                        q_copy(z, j, i).wait_send()
                    n_copy(z, j, i).wait()

    pl.when(core == 0)(lambda: run(True))
    pl.when(core == 1)(lambda: run(False))
    for share_copy in copies:
        share_copy.wait_send()
    tail = out.shape[1] - 8
    counts[...] = out[:, tail, :].astype(jnp.int32)


def radial(range_sq):
    near = lax.rsqrt(range_sq)
    fall = 1.0 / (range_sq * jnp.exp2(range_sq))
    z = 1.0 / (near + KAPPA)
    poly = z * POLY[-1] + POLY[-2]
    for coefficient in POLY[-3::-1]:
        poly = poly * z + coefficient
    return (poly + near) * fall


def compact(rows, places, wide):
    order = lax.broadcasted_iota(jnp.int32, (wide, wide), 0)
    pick = jnp.where(order == places, 1.0, 0.0).astype(jnp.bfloat16)
    return lax.dot_general(
        rows.astype(jnp.bfloat16),
        pick,
        (((1,), (1,)), ((), ())),
        preferred_element_type=jnp.float32,
    )


def plan_items(meta, counts, plan, fields, pieces, tiles):
    f32, bf16, i32 = jnp.float32, jnp.bfloat16, jnp.int32
    blocks = meta.shape[1]
    visits = (meta.shape[0] - 1) // 2
    slots = counts.shape[0]
    height = plan.shape[1]
    spare = tiles * blocks
    held = counts[...].astype(f32).astype(bf16)
    order = lax.broadcasted_iota(i32, (LANES, blocks), 0)
    slot = lax.broadcasted_iota(i32, (slots, blocks), 0)
    active = meta[2 * visits : 2 * visits + 1]
    full, ends, lines = [], [], []
    for visit in range(visits):
        key = meta[visit : visit + 1]
        pick = jnp.where(order == (key & (LANES - 1)), 1.0, 0.0).astype(bf16)
        found = jnp.dot(held, pick, preferred_element_type=f32)
        count = jnp.sum(jnp.where(slot == (key >> 7), found, 0.0), axis=0, keepdims=True)
        count = count.astype(i32)
        line = meta[visits + visit : visits + visit + 1]
        more = count > LANES
        full.append((jnp.where(more, 1, 0), line, line, jnp.full_like(line, LANES)))
        ends.append(jnp.where(more, count - LANES, count))
        lines.append(jnp.where(more, line + 4, line))
    entries = list(full)
    size, at = ends[0], lines[0]
    for visit in range(1, visits):
        end, line = ends[visit], lines[visit]
        both = jnp.minimum(size, 1) * jnp.minimum(end, 1)
        fit = jnp.where(size + end <= LANES, both, 0)
        bigger = end > size
        entries.append(
            (
                both,
                jnp.where((fit == 0) & bigger, line, at),
                line,
                jnp.where(fit > 0, size, LANES),
            )
        )
        take = jnp.where(both > 0, jnp.where(bigger, 0, 1), jnp.where(end > 0, 1, 0))
        at = jnp.where(take > 0, line, at)
        size = jnp.where(fit > 0, 0, jnp.where(take > 0, end, size))
    entries.append((jnp.minimum(size, 1), at, at, jnp.full_like(at, LANES)))
    kinds = len(entries)
    used = kinds * tiles
    for k in range(4):
        fields[k] = jnp.zeros(fields.shape[1:], i32)
    for tile in range(tiles):
        live = jnp.where(active > tile * TILE, 1, 0)
        for j, entry in enumerate(entries):
            row = tile * kinds + j
            fields[0, row : row + 1] = entry[0] * live if tile > 0 else entry[0]
            for k in range(1, 4):
                fields[k, row : row + 1] = entry[k]
    valid = fields[0].astype(f32).astype(bf16)
    below = lax.broadcasted_iota(i32, (blocks, blocks), 0) < lax.broadcasted_iota(
        i32, (blocks, blocks), 1
    )
    below = jnp.where(below, 1.0, 0.0).astype(bf16)
    before = jnp.dot(valid, below, preferred_element_type=f32)
    sums = jnp.dot(valid, jnp.ones((blocks, blocks), bf16), preferred_element_type=f32)
    tall = fields.shape[1]
    under = lax.broadcasted_iota(i32, (tall, tall), 0) > lax.broadcasted_iota(
        i32, (tall, tall), 1
    )
    under = jnp.where(under, 1.0, 0.0).astype(bf16)
    start = jnp.dot(under, sums.astype(bf16), preferred_element_type=f32)
    place = (start + before).astype(i32)
    number = jnp.sum(sums, axis=0, keepdims=True).astype(i32)
    first, second = fields[1], fields[2]
    block_at = lax.broadcasted_iota(i32, (tall, blocks), 1)
    parts = (
        first & 255,
        first >> 8,
        second & 255,
        second >> 8,
        fields[3],
        block_at,
        place // blocks,
        jnp.ones_like(place),
    )
    for k, part in enumerate(parts):
        pieces[k] = part.astype(f32)
    lane = lax.rem(place, blocks)
    fields[0] = jnp.where(fields[0] > 0, lane, -1)
    row = lax.broadcasted_iota(i32, (height, blocks), 0)
    words = [jnp.full((height, blocks), spare * 65536, i32), jnp.zeros((height, blocks), i32)]
    for r in range(used):
        got = compact(pieces[:, r, :], fields[0, r : r + 1], blocks).astype(i32)
        one = got[0:1] + got[1:2] * 256 + (got[5:6] + r // kinds * blocks) * 65536
        two = got[2:3] + got[3:4] * 256 + got[4:5] * 65536
        here = jnp.where(got[7:8] > 0, got[6:7], -1) == row
        words = [jnp.where(here, one, words[0]), jnp.where(here, two, words[1])]
    plan[0, :, 0:blocks] = words[0]
    plan[1, :, 0:blocks] = words[1]
    plan[2, 0:1, 0:blocks] = number
    numbers = lax.broadcasted_iota(i32, (8, blocks), 1).astype(f32)
    for tile in range(1, tiles):
        live = jnp.where(active > tile * TILE, 1.0, 0.0)
        rows = jnp.broadcast_to(live, (8, blocks)).astype(bf16)
        spot = jnp.dot(rows, below, preferred_element_type=f32)[0:1].astype(i32)
        got = compact(numbers, jnp.where(live > 0, spot, -1), blocks).astype(i32)
        total = jnp.dot(rows, jnp.ones((blocks, blocks), bf16), preferred_element_type=f32)
        plan[2, 2 * tile - 1 : 2 * tile, 0:blocks] = got[0:1]
        plan[2, 2 * tile : 2 * tile + 1, 0:blocks] = total[0:1].astype(i32)


def pull_kernel(
    meta, counts, pos, ranks, table, out,
    plan, fields, pieces, items, plan_sem, mixed, sinks, totals,
    later_range, later_weight, later_nodes, last_nodes, next_group, next_nodes,
):
    blocks = meta.shape[1]
    width = pos.shape[2]
    tiles = sinks.shape[0] // blocks
    spare = tiles * blocks
    f32, bf16 = jnp.float32, jnp.bfloat16
    sub8 = lax.broadcasted_iota(jnp.int32, (8, width), 0)
    axis8 = sub8 & 3
    by_rows = (((1,), (1,)), ((), ()))
    order = lax.broadcasted_iota(jnp.int32, (TILE, width), 0)
    lane48 = lax.broadcasted_iota(jnp.int32, (TILE, 48), 1)
    soft_high, soft_rest, soft_last = SOFT
    soft = jnp.where(
        lane48 == 11,
        soft_high,
        jnp.where(lane48 == 27, soft_rest, jnp.where(lane48 == 43, soft_last, 0.0)),
    )

    def axes(first, second, third, fourth, at):
        return jnp.where(at == 0, first, jnp.where(at == 1, second, jnp.where(at == 2, third, fourth)))

    def prepare(block, tile):
        line = [
            jnp.broadcast_to(pos[axis, pl.ds(block, 1), :] * SCALE, (8, width))
            for axis in range(3)
        ]
        norm = line[0] * line[0] + line[1] * line[1] + line[2] * line[2]
        pieces = split(axes(line[0], line[1], line[2], 0.0, axis8) * -2.0)
        norms = split(norm)
        parts = []
        for k in range(3):
            tail = jnp.where(sub8 == 7, norms[k], 1.0 if k == 0 else 0.0)
            parts.append(pieces[k])
            parts.append(jnp.where(sub8 < 3, pieces[k], jnp.where(sub8 == 3, 0.0, tail)))
        wide = jnp.concatenate(parts, axis=0).astype(bf16)
        rank = ranks[pl.ds(block, 1), :]

        at = tile * blocks + block
        pick = jnp.where(order == rank - tile * TILE, 1.0, 0.0).astype(bf16)
        held = lax.dot_general(pick, wide, by_rows, preferred_element_type=f32)
        sinks[at] = (held + soft).astype(bf16)
        totals[at] = jnp.zeros((TILE, LANES), f32)

    def first(step, carry):
        for k in range(4):
            prepare(step * 4 + k, 0)
        return carry

    plan_items(meta, counts, plan, fields, pieces, tiles)
    sinks[spare] = soft.astype(bf16)
    totals[spare] = jnp.zeros((TILE, LANES), f32)
    move = pltpu.make_async_copy(plan, items, plan_sem)
    lax.fori_loop(0, 2, first, 0)
    move.start()
    lax.fori_loop(2, blocks // 4, first, 0)
    move.wait()
    number = items[2, 0, 0]

    def beyond(tile, action):
        def one(step, carry):
            action(items[2, 2 * tile - 1, step], tile)
            return carry

        lax.fori_loop(0, items[2, 2 * tile, 0], one, 0)

    for tile in range(1, tiles):
        beyond(tile, prepare)

    sub = lax.broadcasted_iota(jnp.int32, (8, LANES), 0)
    axis = sub & 3

    lane4 = lax.broadcasted_iota(jnp.int32, (4, LANES), 1)
    bits = blocks.bit_length() - 1
    assert blocks == 1 << bits

    def word(kind, item):
        return items[kind, lax.shift_right_logical(item, bits), item & (blocks - 1)]

    def begin(item, spot):
        code, other = word(0, item), word(1, item)
        shift = other >> 16
        moved = pltpu.roll(table[pl.ds(other & 65535, 4), :], shift & (LANES - 1), 1)
        mixed[spot] = jnp.where(lane4 < shift, table[pl.ds(code & 65535, 4), :], moved)
        row = [jnp.broadcast_to(mixed[spot, f : f + 1, :], (8, LANES)) for f in range(4)]
        norm = row[0] * row[0] + row[1] * row[1] + row[2] * row[2]
        flat = axes(row[0], row[1], row[2], row[3], axis)
        pieces = split(flat)
        norms = split(norm)
        tail = jnp.where(
            sub == 4, norms[0], jnp.where(sub == 5, norms[1], jnp.where(sub == 6, norms[2], 1.0))
        )
        group = jnp.concatenate(
            [
                jnp.where(sub < 4, pieces[0], pieces[1]),
                jnp.where(sub < 3, pieces[2], tail),
            ],
            axis=0,
        ).astype(bf16)
        weighted = split(jnp.where(axis == 3, flat, flat * row[3]))
        moment = jnp.concatenate(
            [
                jnp.where(sub < 4, weighted[0], weighted[1]),
                jnp.where(sub < 4, weighted[2], 0.0),
            ],
            axis=0,
        ).astype(bf16)
        return group, moment

    def reach(item, spot):
        group = next_group[spot]
        return jnp.dot(
            sinks[word(0, item) >> 16],
            jnp.concatenate([group] * 3, axis=0),
            preferred_element_type=f32,
        )

    def weigh(range_sq):
        weight = radial(range_sq)
        high = weight.astype(bf16)
        low = (weight - high.astype(f32)).astype(bf16)
        return jnp.concatenate([high, low], axis=1)

    def gather(weight, moment):
        moment = jnp.concatenate([moment] * 2, axis=1)
        return lax.dot_general(weight, moment, by_rows, preferred_element_type=f32)

    def add(item, pull):
        at = word(0, item) >> 16
        totals[at, :, 0:16] += pull

    for k in range(2 * PAIR):
        next_group[k], later_nodes[k] = begin(k, k)
    for k in range(2 * PAIR):
        later_range[k] = reach(k, k)
    for k in range(2 * PAIR):
        next_group[k], next_nodes[k] = begin(2 * PAIR + k, k)
    for k in range(PAIR):
        later_weight[k] = jnp.zeros(later_weight.shape[1:], bf16)
        last_nodes[k] = jnp.zeros(last_nodes.shape[1:], bf16)

    def main(step, carry):
        base = step * (2 * PAIR)
        before = [gather(later_weight[k], last_nodes[k]) for k in range(PAIR)]
        after = [reach(base + 2 * PAIR + k, k) for k in range(2 * PAIR)]
        now = [gather(weigh(later_range[k]), later_nodes[k]) for k in range(PAIR)]
        for k in range(PAIR):
            add(jnp.where(step > 0, base - PAIR + k, number), before[k])
        for k in range(PAIR):
            later_weight[k] = weigh(later_range[PAIR + k])
            last_nodes[k] = later_nodes[PAIR + k]
        for k in range(PAIR):
            add(base + k, now[k])
        fresh = [begin(base + 4 * PAIR + k, k) for k in range(2 * PAIR)]
        for k in range(2 * PAIR):
            later_range[k] = after[k]
            later_nodes[k] = next_nodes[k]
            next_group[k], next_nodes[k] = fresh[k]
        return carry

    groups = (number + PAIR - 1) // PAIR
    lax.fori_loop(0, groups // 2 + 1, main, 0)

    lane16 = lax.broadcasted_iota(jnp.int32, (TILE, LANES), 1)
    wide_tile = -(-TILE // LANES) * LANES

    def laid(flat, block, tile):
        flat = flat[0:4] + flat[4:8] + flat[8:12]
        flat = jnp.concatenate([flat, flat], axis=0)
        rank = jnp.broadcast_to(ranks[pl.ds(block, 1), :] - tile * TILE, (8, width))
        parts = []
        for k in range(0, width, LANES):
            at = rank[:, k : k + LANES]
            low = at & (LANES - 1)
            part = jnp.zeros((8, LANES), f32)
            for j in range(0, wide_tile, LANES):
                piece = jnp.take_along_axis(
                    flat[:, j : j + LANES], low, axis=1, mode="promise_in_bounds"
                )
                here = (at >= j) & (at < min(j + LANES, TILE))
                part = jnp.where(here, piece, part)
            parts.append(part)
        return jnp.concatenate(parts, axis=1)

    def turn(value):
        value = jnp.concatenate(
            [value, jnp.zeros((wide_tile - TILE, LANES), f32)], axis=0
        )
        return jnp.transpose(value)

    def store(block, sums):
        for axis in range(3):
            there = pos[axis, pl.ds(block, 1), :] * SCALE
            out[axis, pl.ds(block, 1), :] = sums[axis : axis + 1] - sums[3:4] * there

    def last(step, carry):
        packed = totals[step * 8]
        for k in range(1, 8):
            moved = pltpu.roll(totals[step * 8 + k], 16 * k, 1)
            packed = jnp.where(lane16 < 16 * k, packed, moved)
        turned = turn(packed)
        for k in range(8):
            store(step * 8 + k, laid(turned[16 * k : 16 * k + 16], step * 8 + k, 0))
        return carry

    lax.fori_loop(0, blocks // 8, last, 0)

    def rest(block, tile):
        sums = laid(turn(totals[tile * blocks + block])[0:16], block, tile)
        for axis in range(3):
            there = pos[axis, pl.ds(block, 1), :] * SCALE
            out[axis, pl.ds(block, 1), :] += sums[axis : axis + 1] - sums[3:4] * there

    for tile in range(1, tiles):
        beyond(tile, rest)


def pull_call(meta, counts, pos, ranks, table):
    blocks, width = ranks.shape
    visits = (meta.shape[0] - 1) // 2
    tiles = -(-width // TILE)
    spare = tiles * blocks
    kinds = -(-2 * visits * tiles // 8) * 8
    height = -(-(2 * visits * tiles * blocks + 12 * PAIR) // (8 * blocks)) * 8
    scratch = [
        pltpu.VMEM((3, height, LANES), jnp.int32),
        pltpu.VMEM((4, kinds, blocks), jnp.int32),
        pltpu.VMEM((8, kinds, blocks), jnp.float32),
        pltpu.SMEM((3, height, LANES), jnp.int32),
        pltpu.SemaphoreType.DMA,
        pltpu.VMEM((2 * PAIR, 4, LANES), jnp.float32),
        pltpu.VMEM((spare + 1, TILE, 48), jnp.bfloat16),
        pltpu.VMEM((spare + 1, TILE, LANES), jnp.float32),
        pltpu.VMEM((2 * PAIR, TILE, LANES), jnp.float32),
        pltpu.VMEM((PAIR, TILE, 2 * LANES), jnp.bfloat16),
        pltpu.VMEM((2 * PAIR, 16, LANES), jnp.bfloat16),
        pltpu.VMEM((PAIR, 16, LANES), jnp.bfloat16),
        pltpu.VMEM((2 * PAIR, 16, LANES), jnp.bfloat16),
        pltpu.VMEM((2 * PAIR, 16, LANES), jnp.bfloat16),
    ]
    vmem = pl.BlockSpec(memory_space=pltpu.VMEM)
    return pl.pallas_call(
        pull_kernel,
        out_shape=jax.ShapeDtypeStruct((3, blocks, width), jnp.float32),
        in_specs=[vmem] * 5,
        out_specs=vmem,
        scratch_shapes=scratch,
        compiler_params=pltpu.CompilerParams(vmem_limit_bytes=36 * 1024 * 1024),
    )(meta, counts, pos, ranks, table)


def local(
    positions,
    time_bins,
    home_groups,
    targets,
    target_groups,
    node_pos,
    node_mass,
    node_lists,
    list_counts,
):
    domains = lax.axis_size("dom")
    sharers = lax.axis_size("sub")
    devices = domains * sharers
    blocks, most = targets.shape
    width = positions.shape[2]
    groups, length = node_lists.shape
    share = groups // sharers
    stride = share * 8 + 8
    per_device = node_mass.shape[0]
    height = per_device // LANES
    f32, i32 = jnp.float32, jnp.int32
    vmem = pl.BlockSpec(memory_space=pltpu.VMEM)
    dma = pltpu.SemaphoreType.DMA

    hbm = pl.BlockSpec(memory_space=pltpu.HBM)
    deep, wide = domains // 2, sharers // 2
    most_first = max(2, wide)
    table, counts, ranks, meta, pos = pl.pallas_call(
        functools.partial(domain_kernel, groups=groups, share=share, stride=stride),
        out_shape=[
            jax.ShapeDtypeStruct((devices, stride, LANES), f32),
            jax.ShapeDtypeStruct((devices, LANES), i32),
            jax.ShapeDtypeStruct((blocks, width), i32),
            jax.ShapeDtypeStruct((2 * most + 3, blocks), i32),
            jax.ShapeDtypeStruct((3, blocks, width), f32),
        ],
        in_specs=[hbm] * 9,
        out_specs=[vmem] * 5,
        scratch_shapes=[
            pltpu.VMEM((3, per_device), f32),
            pltpu.VMEM((height, LANES), f32),
            pltpu.VMEM((blocks, width), i32),
            pltpu.VMEM((1, blocks), i32),
            pltpu.VMEM((most, blocks), i32),
            pltpu.VMEM((most, blocks), i32),
            pltpu.VMEM((groups, length), i32),
            pltpu.VMEM((sharers, 3, per_device), f32),
            pltpu.VMEM((sharers, height, LANES), f32),
            pltpu.VMEM((sharers * height * 4, LANES), f32),
            pltpu.VMEM((stride, LANES), f32),
            pltpu.SMEM((groups,), i32),
            dma((9,)),
        ]
        + [dma((2, sharers - 1))] * 2
        + [dma((deep,))] * 2
        + [dma((deep, deep))]
        + [dma((deep, most_first))] * 2
        + [dma((deep, most_first, most_first))] * 2
        + [dma((deep, 2, wide))] * 2,
        compiler_params=pltpu.CompilerParams(
            collective_id=0, has_side_effects=True, vmem_limit_bytes=24 * 1024 * 1024
        ),
    )(
        *(
            pltpu.with_memory_space_constraint(array, pltpu.HBM)
            for array in (
                node_pos,
                node_mass.reshape(height, LANES),
                time_bins,
                home_groups.reshape(1, blocks),
                targets.T,
                target_groups.T,
                node_lists,
                jnp.transpose(positions, (1, 0, 2)),
                list_counts,
            )
        )
    )
    forces = pull_call(
        meta,
        counts,
        pos,
        ranks,
        table.reshape(-1, LANES),
    )
    return jnp.transpose(forces, (1, 0, 2))


def solution(mesh):
    return jax.shard_map(
        local,
        mesh=mesh,
        in_specs=(
            P(("dom", "sub"), None, None),
            P(("dom", "sub"), None),
            P(("dom", "sub")),
            P(("dom", "sub"), None),
            P(("dom", "sub"), None),
            P(None, ("dom", "sub")),
            P(("dom", "sub")),
            P("dom", None),
            P("dom"),
        ),
        out_specs=P(("dom", "sub"), None, None),
        check_vma=False,
    )
```

```python
import functools
import math

import jax
import jax.numpy as jnp
from jax import lax
from jax.experimental import pallas as pl
from jax.experimental.pallas import tpu as pltpu
from jax.sharding import PartitionSpec as P

CUR_BIN = 2
SOFTEN_SQ = 0.04
LANES = 128
SCALE = math.sqrt(math.log2(math.e) / 4)
KAPPA = 0.5033782057491644
LEAD = 1.0644227815066034
POLY = (
    0.0006822818085192818,
    0.6891780368303475,
    -0.07494018001023989,
    -0.03418881002810906,
    0.008589076872810486,
)
MASS_SCALE = LEAD * SCALE / math.sqrt(math.pi)
MESH = pl.DeviceIdType.MESH
TILE = 144
PAIR = 3


def bf16_pieces(value):
    pieces = []
    for _ in range(3):
        mantissa, exponent = math.frexp(value)
        piece = math.ldexp(round(mantissa * 256), exponent - 8)
        pieces.append(piece)
        value -= piece
    return tuple(pieces)


SOFT = bf16_pieces(SOFTEN_SQ * SCALE * SCALE)


def split(value):
    high = value.astype(jnp.bfloat16).astype(jnp.float32)
    rest = value - high
    middle = rest.astype(jnp.bfloat16).astype(jnp.float32)
    return value, rest, rest - middle


def axes(first, second, third, fourth, at):
    return jnp.where(at == 0, first, jnp.where(at == 1, second, jnp.where(at == 2, third, fourth)))


def soft_row():
    lane48 = lax.broadcasted_iota(jnp.int32, (TILE, 48), 1)
    soft_high, soft_rest, soft_last = SOFT
    return jnp.where(
        lane48 == 11,
        soft_high,
        jnp.where(lane48 == 27, soft_rest, jnp.where(lane48 == 43, soft_last, 0.0)),
    )


def block_sinks(pos, ranks, block, tile):
    width = pos.shape[2]
    f32, bf16 = jnp.float32, jnp.bfloat16
    sub8 = lax.broadcasted_iota(jnp.int32, (8, width), 0)
    axis8 = sub8 & 3
    order = lax.broadcasted_iota(jnp.int32, (TILE, width), 0)
    line = [
        jnp.broadcast_to(pos[axis, pl.ds(block, 1), :] * SCALE, (8, width))
        for axis in range(3)
    ]
    norm = line[0] * line[0] + line[1] * line[1] + line[2] * line[2]
    pieces = split(axes(line[0], line[1], line[2], 0.0, axis8) * -2.0)
    norms = split(norm)
    parts = []
    for k in range(3):
        tail = jnp.where(sub8 == 7, norms[k], 1.0 if k == 0 else 0.0)
        parts.append(pieces[k])
        parts.append(jnp.where(sub8 < 3, pieces[k], jnp.where(sub8 == 3, 0.0, tail)))
    wide = jnp.concatenate(parts, axis=0).astype(bf16)
    rank = ranks[pl.ds(block, 1), :]
    pick = jnp.where(order == rank - tile * TILE, 1.0, 0.0).astype(bf16)
    held = lax.dot_general(
        pick, wide, (((1,), (1,)), ((), ())), preferred_element_type=f32
    )
    return (held + soft_row()).astype(bf16)


def fill_ranks(bins, ranks, meta):
    blocks, width = bins.shape
    last = meta.shape[0] - 1
    active = bins[...] <= CUR_BIN
    flags = jnp.where(active, 1.0, 0.0).astype(jnp.bfloat16)
    upper = lax.broadcasted_iota(jnp.int32, (width, width), 0) <= lax.broadcasted_iota(
        jnp.int32, (width, width), 1
    )
    running = jnp.dot(
        flags,
        jnp.where(upper, 1.0, 0.0).astype(jnp.bfloat16),
        preferred_element_type=jnp.float32,
    ).astype(jnp.int32)
    ranks[...] = jnp.where(active, running - 1, -1)
    number = lax.dot_general(
        jnp.ones((8, width), jnp.bfloat16),
        flags,
        (((1,), (1,)), ((), ())),
        preferred_element_type=jnp.float32,
    ).astype(jnp.int32)
    meta[last : last + 1] = number[0:1]


def fill_places(homes, targets, target_groups, meta, groups, share, stride):
    domain = lax.axis_index("dom")
    most = targets.shape[0]
    holders = groups // share

    def places(owner, group):
        slot = owner * holders + lax.div(group, share)
        inner = lax.rem(group, share)
        return slot * LANES + inner, slot * stride + inner * 8

    key, line = places(domain, homes[...])
    meta[0:1] = key
    meta[most + 1 : most + 2] = line
    key, line = places(jnp.maximum(targets[...], 0), target_groups[...])
    meta[1 : most + 1] = jnp.where(targets[...] >= 0, key, LANES - 1)
    meta[most + 2 : 2 * most + 2] = line


def gather_lists(all_pos, all_mass, lists, list_counts, out, stack):
    sharers, _, per_device = all_pos.shape
    height = per_device // LANES
    total, length = lists.shape
    share = total // sharers
    place = lax.axis_index("sub")
    f32, bf16 = jnp.float32, jnp.bfloat16
    for owner in range(sharers):
        for high in range(height):
            at = (owner * height + high) * 4
            stack[at : at + 3] = all_pos[owner, :, high * LANES : (high + 1) * LANES] * SCALE
            stack[at + 3 : at + 4] = all_mass[owner, high : high + 1, :] * MASS_SCALE
    half = sharers * height // 2
    rows = half * 4
    pieces = [
        piece.astype(bf16)
        for piece in split(jnp.concatenate([stack[0:rows], stack[rows : 2 * rows]], axis=1))
    ]
    order = lax.broadcasted_iota(jnp.int32, (2 * LANES, length), 0)
    pair = lax.broadcasted_iota(jnp.int32, (8, length), 0) >> 2
    lane = lax.broadcasted_iota(jnp.int32, (4, length), 1)
    axis = lax.broadcasted_iota(jnp.int32, (4, length), 0)

    def one(local):
        group = place * share + local
        index = lists[pl.ds(group, 1), :]
        high = index >> 7
        far = jnp.where(high >= half, 1, 0)
        low = (index & (LANES - 1)) + far * LANES
        high = jnp.broadcast_to(high - far * half, (8, length)) - pair
        pick = jnp.where(order == low, 1.0, 0.0).astype(bf16)
        found = sum(jnp.dot(piece, pick, preferred_element_type=f32) for piece in pieces)
        total = jnp.zeros((8, length), f32)
        for t in range(rows // 8):
            total = jnp.where(high == 2 * t, found[8 * t : 8 * t + 8], total)
        picked = total[0:4] + total[4:8]
        valid = (axis < 3) | (lane < list_counts[group])
        picked = jnp.where(valid, picked, 0.0)
        out[pl.ds(pl.multiple_of(local * 8, 8), 8), :] = jnp.concatenate(
            [picked[:, 0:LANES], picked[:, LANES : 2 * LANES]], axis=0
        )

    def some(step, carry):
        for k in range(2):
            one(step * 2 + k)
        return carry

    lax.fori_loop(0, share // 2, some, 0)
    lane8 = lax.broadcasted_iota(jnp.int32, (8, LANES), 1)
    tail = jnp.zeros((8, LANES), jnp.int32)
    for local in range(share):
        tail = jnp.where(lane8 == local, list_counts[place * share + local], tail)
    out[share * 8 : share * 8 + 8, :] = tail.astype(f32)


def domain_kernel(
    node_pos, node_mass, bins, homes, targets, target_groups, lists, positions, list_counts,
    out, counts, ranks, meta, pos, sinks,
    own_pos, own_mass, own_bins, own_homes, own_targets, own_groups, own_lists,
    all_pos, all_mass, stack, own, own_counts,
    load_sem, s_send, s_recv, z_send, z_recv, f_send, p_send, p_recv, q_send, q_recv,
    n_send, n_recv, groups, share, stride,
):
    sharers, domains = lax.axis_size("sub"), lax.axis_size("dom")
    domain, place = lax.axis_index("dom"), lax.axis_index("sub")
    deep, wide = domains // 2, sharers // 2
    half = deep // 2
    core = lax.rem(place, 2)
    across = place // 2
    layer, side = domain // 2, lax.rem(domain, 2)
    upper = layer // half
    gate = (1 - upper) * half + upper * (half - 1)
    other_gate = (1 - upper) * (half - 1) + upper * half
    sibling = {"sub": place + 1 - 2 * core}
    barrier = pltpu.get_barrier_semaphore()

    def shifted(at, by, size):
        return lax.rem(at + by + size, size)

    def device(z, dy, dx):
        return {
            "dom": z * 2 + shifted(side, dy, 2),
            "sub": shifted(across, dx, wide) * 2 + core,
        }

    def slot(z, dy, dx):
        there = device(z, -dy, -dx)
        return there["dom"] * sharers + there["sub"]

    others = [{"sub": lax.rem(place + k, sharers)} for k in range(1, sharers)]
    peers = [device(shifted(layer, k, deep), 0, 0) for k in range(1, deep)]
    peers += [device(layer, 1, 0)] + others
    for peer in peers:
        pl.semaphore_signal(barrier, inc=1, device_id=peer, device_id_type=MESH)
    loads = [
        pltpu.make_async_copy(source, target, load_sem.at[k])
        for k, (source, target) in enumerate(
            (
                (node_pos, own_pos),
                (node_mass, own_mass),
                (bins, own_bins),
                (homes, own_homes),
                (targets, own_targets),
                (target_groups, own_groups),
                (lists, own_lists),
                (positions, pos),
                (list_counts, own_counts),
            )
        )
    ]
    for load in loads:
        load.start()
    for load in loads[:2]:
        load.wait()
    pl.semaphore_wait(barrier, len(peers))
    copies = []
    for k, other in enumerate(others):
        for j, (source, target) in enumerate(((own_pos, all_pos), (own_mass, all_mass))):
            share_copy = pltpu.make_async_remote_copy(
                src_ref=source,
                dst_ref=target.at[place],
                send_sem=s_send.at[j, k],
                recv_sem=s_recv.at[j, k],
                device_id=other,
                device_id_type=MESH,
            )
            share_copy.start()
            copies.append(share_copy)
    all_pos[place] = own_pos[...]
    all_mass[place] = own_mass[...]
    for load in loads[2:]:
        load.wait()
    fill_ranks(own_bins, ranks, meta)

    def prepare(step, carry):
        for k in range(4):
            sinks[step * 4 + k] = block_sinks(pos, ranks, step * 4 + k, 0)
        return carry

    lax.fori_loop(0, sinks.shape[0] // 4, prepare, 0)
    for share_copy in copies:
        share_copy.wait_recv()
    gather_lists(all_pos, all_mass, own_lists, own_counts, own, stack)
    fill_places(own_homes, own_targets, own_groups, meta, groups, share, stride)

    def run(side_first):
        first, second = (2, wide) if side_first else (wide, 2)

        def cell(j, i):
            return (j, i) if side_first else (i, j)

        def copy(source, at, send, recv, there):
            return pltpu.make_async_remote_copy(
                src_ref=source,
                dst_ref=out.at[at],
                send_sem=send,
                recv_sem=recv,
                device_id=there,
                device_id_type=MESH,
            )

        mine = slot(layer, 0, 0)

        def z_copy(k, to):
            return copy(own, mine, z_send.at[k], z_recv.at[layer], device(to, 0, 0))

        def z_wait(z):
            copy(own, slot(z, 0, 0), z_send.at[0], z_recv.at[z], device(z, 0, 0)).wait_recv()

        def f_copy(z, k):
            to = upper * half + lax.rem(layer - upper * half + k, half)
            at = slot(z, 0, 0)
            return copy(
                out.at[at], at, f_send.at[lax.rem(z, half), k], z_recv.at[z], device(to, 0, 0)
            )

        def p_copy(z, j, source=None):
            at = slot(z, 0, 0)
            return copy(
                out.at[at] if source is None else source,
                at,
                p_send.at[z, j],
                p_recv.at[z, j],
                device(layer, *cell(j, 0)),
            )

        def q_copy(z, j, i, source=None):
            at = slot(z, *cell(j, 0))
            return copy(
                out.at[at] if source is None else source,
                at,
                q_send.at[z, j, i],
                q_recv.at[z, j, i],
                device(layer, *cell(0, i)),
            )

        def n_copy(z, j, i, source=None):
            c = cell(j, i)
            at = slot(z, *c)
            return copy(
                out.at[at] if source is None else source,
                at,
                n_send.at[(z,) + c],
                n_recv.at[(z,) + c],
                sibling,
            )

        def after_z(z, source=None):
            for j in range(1, first):
                p_copy(z, j, source).start()
            for i in range(1, second):
                q_copy(z, 0, i, source).start()
            n_copy(z, 0, 0, source).start()

        def take_z(z):
            z_wait(z)

            @pl.when((layer == other_gate) & (z // half != upper))
            def _():
                for k in range(1, half):
                    f_copy(z, k).start()

            after_z(z)

        def take_p(z):
            for j in range(1, first):
                p_copy(z, j).wait_recv()
                for i in range(1, second):
                    q_copy(z, j, i).start()
                n_copy(z, j, 0).start()

        def take_q(z):
            for j in range(first):
                for i in range(1, second):
                    q_copy(z, j, i).wait_recv()
                    n_copy(z, j, i).start()

        def at_distance(k, action):
            pl.when(layer + k < deep)(lambda: action(layer + k))
            pl.when(layer - k >= 0)(lambda: action(layer - k))

        for k in range(1, half):
            z_copy(k, upper * half + lax.rem(layer - upper * half + k, half)).start()
        z_copy(0, gate).start()
        after_z(layer, own)
        out[mine] = own[...]
        take_p(layer)
        for k in range(1, deep):
            at_distance(k, take_z)
            if k > 1:
                at_distance(k - 1, take_p)
        at_distance(deep - 1, take_p)
        take_q(layer)
        for k in range(1, deep):
            at_distance(k, take_q)
        for k in range(half):
            z_copy(k, gate).wait_send()

        @pl.when(layer == other_gate)
        def _():
            for z in range(half):
                for k in range(1, half):
                    f_copy(z, k).wait_send()

        for z in range(deep):
            for j in range(first):
                for i in range(second):
                    if i == 0 and j > 0:
                        p_copy(z, j).wait_send()
                    if i > 0:
                        q_copy(z, j, i).wait_send()
                    n_copy(z, j, i).wait()

    pl.when(core == 0)(lambda: run(True))
    pl.when(core == 1)(lambda: run(False))
    for share_copy in copies:
        share_copy.wait_send()
    tail = out.shape[1] - 8
    counts[...] = out[:, tail, :].astype(jnp.int32)


def radial(range_sq):
    near = lax.rsqrt(range_sq)
    fall = 1.0 / (range_sq * jnp.exp2(range_sq))
    z = 1.0 / (near + KAPPA)
    poly = z * POLY[-1] + POLY[-2]
    for coefficient in POLY[-3::-1]:
        poly = poly * z + coefficient
    return (poly + near) * fall


def compact(rows, places, wide):
    order = lax.broadcasted_iota(jnp.int32, (wide, wide), 0)
    pick = jnp.where(order == places, 1.0, 0.0).astype(jnp.bfloat16)
    return lax.dot_general(
        rows.astype(jnp.bfloat16),
        pick,
        (((1,), (1,)), ((), ())),
        preferred_element_type=jnp.float32,
    )


def plan_items(meta, counts, plan, fields, pieces, tiles):
    f32, bf16, i32 = jnp.float32, jnp.bfloat16, jnp.int32
    blocks = meta.shape[1]
    visits = (meta.shape[0] - 1) // 2
    slots = counts.shape[0]
    height = plan.shape[1]
    spare = tiles * blocks
    held = counts[...].astype(f32).astype(bf16)
    order = lax.broadcasted_iota(i32, (LANES, blocks), 0)
    slot = lax.broadcasted_iota(i32, (slots, blocks), 0)
    active = meta[2 * visits : 2 * visits + 1]
    full, ends, lines = [], [], []
    for visit in range(visits):
        key = meta[visit : visit + 1]
        pick = jnp.where(order == (key & (LANES - 1)), 1.0, 0.0).astype(bf16)
        found = jnp.dot(held, pick, preferred_element_type=f32)
        count = jnp.sum(jnp.where(slot == (key >> 7), found, 0.0), axis=0, keepdims=True)
        count = count.astype(i32)
        line = meta[visits + visit : visits + visit + 1]
        more = count > LANES
        full.append((jnp.where(more, 1, 0), line, line, jnp.full_like(line, LANES)))
        ends.append(jnp.where(more, count - LANES, count))
        lines.append(jnp.where(more, line + 4, line))
    entries = list(full)
    size, at = ends[0], lines[0]
    for visit in range(1, visits):
        end, line = ends[visit], lines[visit]
        both = jnp.minimum(size, 1) * jnp.minimum(end, 1)
        fit = jnp.where(size + end <= LANES, both, 0)
        bigger = end > size
        entries.append(
            (
                both,
                jnp.where((fit == 0) & bigger, line, at),
                line,
                jnp.where(fit > 0, size, LANES),
            )
        )
        take = jnp.where(both > 0, jnp.where(bigger, 0, 1), jnp.where(end > 0, 1, 0))
        at = jnp.where(take > 0, line, at)
        size = jnp.where(fit > 0, 0, jnp.where(take > 0, end, size))
    entries.append((jnp.minimum(size, 1), at, at, jnp.full_like(at, LANES)))
    kinds = len(entries)
    used = kinds * tiles
    for k in range(4):
        fields[k] = jnp.zeros(fields.shape[1:], i32)
    for tile in range(tiles):
        live = jnp.where(active > tile * TILE, 1, 0)
        for j, entry in enumerate(entries):
            row = tile * kinds + j
            fields[0, row : row + 1] = entry[0] * live if tile > 0 else entry[0]
            for k in range(1, 4):
                fields[k, row : row + 1] = entry[k]
    valid = fields[0].astype(f32).astype(bf16)
    below = lax.broadcasted_iota(i32, (blocks, blocks), 0) < lax.broadcasted_iota(
        i32, (blocks, blocks), 1
    )
    below = jnp.where(below, 1.0, 0.0).astype(bf16)
    before = jnp.dot(valid, below, preferred_element_type=f32)
    sums = jnp.dot(valid, jnp.ones((blocks, blocks), bf16), preferred_element_type=f32)
    tall = fields.shape[1]
    under = lax.broadcasted_iota(i32, (tall, tall), 0) > lax.broadcasted_iota(
        i32, (tall, tall), 1
    )
    under = jnp.where(under, 1.0, 0.0).astype(bf16)
    start = jnp.dot(under, sums.astype(bf16), preferred_element_type=f32)
    place = (start + before).astype(i32)
    number = jnp.sum(sums, axis=0, keepdims=True).astype(i32)
    first, second = fields[1], fields[2]
    block_at = lax.broadcasted_iota(i32, (tall, blocks), 1)
    parts = (
        first & 255,
        first >> 8,
        second & 255,
        second >> 8,
        fields[3],
        block_at,
        place // blocks,
        jnp.ones_like(place),
    )
    for k, part in enumerate(parts):
        pieces[k] = part.astype(f32)
    lane = lax.rem(place, blocks)
    fields[0] = jnp.where(fields[0] > 0, lane, -1)
    row = lax.broadcasted_iota(i32, (height, blocks), 0)
    words = [jnp.full((height, blocks), spare * 65536, i32), jnp.zeros((height, blocks), i32)]
    for r in range(used):
        got = compact(pieces[:, r, :], fields[0, r : r + 1], blocks).astype(i32)
        one = got[0:1] + got[1:2] * 256 + (got[5:6] + r // kinds * blocks) * 65536
        two = got[2:3] + got[3:4] * 256 + got[4:5] * 65536
        here = jnp.where(got[7:8] > 0, got[6:7], -1) == row
        words = [jnp.where(here, one, words[0]), jnp.where(here, two, words[1])]
    plan[0, :, 0:blocks] = words[0]
    plan[1, :, 0:blocks] = words[1]
    plan[2, 0:1, 0:blocks] = number
    numbers = lax.broadcasted_iota(i32, (8, blocks), 1).astype(f32)
    for tile in range(1, tiles):
        live = jnp.where(active > tile * TILE, 1.0, 0.0)
        rows = jnp.broadcast_to(live, (8, blocks)).astype(bf16)
        spot = jnp.dot(rows, below, preferred_element_type=f32)[0:1].astype(i32)
        got = compact(numbers, jnp.where(live > 0, spot, -1), blocks).astype(i32)
        total = jnp.dot(rows, jnp.ones((blocks, blocks), bf16), preferred_element_type=f32)
        plan[2, 2 * tile - 1 : 2 * tile, 0:blocks] = got[0:1]
        plan[2, 2 * tile : 2 * tile + 1, 0:blocks] = total[0:1].astype(i32)


def pull_kernel(
    meta, counts, pos, ranks, own_sinks, table, out,
    plan, fields, pieces, items, plan_sem, mixed, sinks, totals,
    later_range, later_weight, later_nodes, last_nodes, next_group, next_nodes,
):
    blocks = meta.shape[1]
    width = pos.shape[2]
    tiles = sinks.shape[0] // blocks
    spare = tiles * blocks
    f32, bf16 = jnp.float32, jnp.bfloat16
    by_rows = (((1,), (1,)), ((), ()))

    def prepare(block, tile):
        at = tile * blocks + block
        sinks[at] = block_sinks(pos, ranks, block, tile)
        totals[at] = jnp.zeros((TILE, LANES), f32)

    def first(step, carry):
        for k in range(4):
            block = step * 4 + k
            sinks[block] = own_sinks[block]
            totals[block] = jnp.zeros((TILE, LANES), f32)
        return carry

    plan_items(meta, counts, plan, fields, pieces, tiles)
    sinks[spare] = soft_row().astype(bf16)
    totals[spare] = jnp.zeros((TILE, LANES), f32)
    move = pltpu.make_async_copy(plan, items, plan_sem)
    lax.fori_loop(0, 2, first, 0)
    move.start()
    lax.fori_loop(2, blocks // 4, first, 0)
    move.wait()
    number = items[2, 0, 0]

    def beyond(tile, action):
        def one(step, carry):
            action(items[2, 2 * tile - 1, step], tile)
            return carry

        lax.fori_loop(0, items[2, 2 * tile, 0], one, 0)

    for tile in range(1, tiles):
        beyond(tile, prepare)

    sub = lax.broadcasted_iota(jnp.int32, (8, LANES), 0)
    axis = sub & 3

    lane4 = lax.broadcasted_iota(jnp.int32, (4, LANES), 1)
    bits = blocks.bit_length() - 1
    assert blocks == 1 << bits

    def word(kind, item):
        return items[kind, lax.shift_right_logical(item, bits), item & (blocks - 1)]

    def begin(item, spot):
        code, other = word(0, item), word(1, item)
        shift = other >> 16
        moved = pltpu.roll(table[pl.ds(other & 65535, 4), :], shift & (LANES - 1), 1)
        mixed[spot] = jnp.where(lane4 < shift, table[pl.ds(code & 65535, 4), :], moved)
        row = [jnp.broadcast_to(mixed[spot, f : f + 1, :], (8, LANES)) for f in range(4)]
        norm = row[0] * row[0] + row[1] * row[1] + row[2] * row[2]
        flat = axes(row[0], row[1], row[2], row[3], axis)
        pieces = split(flat)
        norms = split(norm)
        tail = jnp.where(
            sub == 4, norms[0], jnp.where(sub == 5, norms[1], jnp.where(sub == 6, norms[2], 1.0))
        )
        group = jnp.concatenate(
            [
                jnp.where(sub < 4, pieces[0], pieces[1]),
                jnp.where(sub < 3, pieces[2], tail),
            ],
            axis=0,
        ).astype(bf16)
        weighted = split(jnp.where(axis == 3, flat, flat * row[3]))
        moment = jnp.concatenate(
            [
                jnp.where(sub < 4, weighted[0], weighted[1]),
                jnp.where(sub < 4, weighted[2], 0.0),
            ],
            axis=0,
        ).astype(bf16)
        return group, moment

    def reach(item, spot):
        group = next_group[spot]
        return jnp.dot(
            sinks[word(0, item) >> 16],
            jnp.concatenate([group] * 3, axis=0),
            preferred_element_type=f32,
        )

    def weigh(range_sq):
        weight = radial(range_sq)
        high = weight.astype(bf16)
        low = (weight - high.astype(f32)).astype(bf16)
        return jnp.concatenate([high, low], axis=1)

    def gather(weight, moment):
        moment = jnp.concatenate([moment] * 2, axis=1)
        return lax.dot_general(weight, moment, by_rows, preferred_element_type=f32)

    def add(item, pull):
        at = word(0, item) >> 16
        totals[at, :, 0:16] += pull

    for k in range(2 * PAIR):
        next_group[k], later_nodes[k] = begin(k, k)
    for k in range(2 * PAIR):
        later_range[k] = reach(k, k)
    for k in range(2 * PAIR):
        next_group[k], next_nodes[k] = begin(2 * PAIR + k, k)
    for k in range(PAIR):
        later_weight[k] = jnp.zeros(later_weight.shape[1:], bf16)
        last_nodes[k] = jnp.zeros(last_nodes.shape[1:], bf16)

    def main(step, carry):
        base = step * (2 * PAIR)
        before = [gather(later_weight[k], last_nodes[k]) for k in range(PAIR)]
        after = [reach(base + 2 * PAIR + k, k) for k in range(2 * PAIR)]
        now = [gather(weigh(later_range[k]), later_nodes[k]) for k in range(PAIR)]
        for k in range(PAIR):
            add(jnp.where(step > 0, base - PAIR + k, number), before[k])
        for k in range(PAIR):
            later_weight[k] = weigh(later_range[PAIR + k])
            last_nodes[k] = later_nodes[PAIR + k]
        for k in range(PAIR):
            add(base + k, now[k])
        fresh = [begin(base + 4 * PAIR + k, k) for k in range(2 * PAIR)]
        for k in range(2 * PAIR):
            later_range[k] = after[k]
            later_nodes[k] = next_nodes[k]
            next_group[k], next_nodes[k] = fresh[k]
        return carry

    groups = (number + PAIR - 1) // PAIR
    lax.fori_loop(0, groups // 2 + 1, main, 0)

    lane16 = lax.broadcasted_iota(jnp.int32, (TILE, LANES), 1)
    wide_tile = -(-TILE // LANES) * LANES

    def laid(flat, block, tile):
        flat = flat[0:4] + flat[4:8] + flat[8:12]
        flat = jnp.concatenate([flat, flat], axis=0)
        rank = jnp.broadcast_to(ranks[pl.ds(block, 1), :] - tile * TILE, (8, width))
        parts = []
        for k in range(0, width, LANES):
            at = rank[:, k : k + LANES]
            low = at & (LANES - 1)
            part = jnp.zeros((8, LANES), f32)
            for j in range(0, wide_tile, LANES):
                piece = jnp.take_along_axis(
                    flat[:, j : j + LANES], low, axis=1, mode="promise_in_bounds"
                )
                here = (at >= j) & (at < min(j + LANES, TILE))
                part = jnp.where(here, piece, part)
            parts.append(part)
        return jnp.concatenate(parts, axis=1)

    def turn(value):
        value = jnp.concatenate(
            [value, jnp.zeros((wide_tile - TILE, LANES), f32)], axis=0
        )
        return jnp.transpose(value)

    def store(block, sums):
        for axis in range(3):
            there = pos[axis, pl.ds(block, 1), :] * SCALE
            out[axis, pl.ds(block, 1), :] = sums[axis : axis + 1] - sums[3:4] * there

    def last(step, carry):
        packed = totals[step * 8]
        for k in range(1, 8):
            moved = pltpu.roll(totals[step * 8 + k], 16 * k, 1)
            packed = jnp.where(lane16 < 16 * k, packed, moved)
        turned = turn(packed)
        for k in range(8):
            store(step * 8 + k, laid(turned[16 * k : 16 * k + 16], step * 8 + k, 0))
        return carry

    lax.fori_loop(0, blocks // 8, last, 0)

    def rest(block, tile):
        sums = laid(turn(totals[tile * blocks + block])[0:16], block, tile)
        for axis in range(3):
            there = pos[axis, pl.ds(block, 1), :] * SCALE
            out[axis, pl.ds(block, 1), :] += sums[axis : axis + 1] - sums[3:4] * there

    for tile in range(1, tiles):
        beyond(tile, rest)


def pull_call(meta, counts, pos, ranks, sinks, table):
    blocks, width = ranks.shape
    visits = (meta.shape[0] - 1) // 2
    tiles = -(-width // TILE)
    spare = tiles * blocks
    kinds = -(-2 * visits * tiles // 8) * 8
    height = -(-(2 * visits * tiles * blocks + 12 * PAIR) // (8 * blocks)) * 8
    scratch = [
        pltpu.VMEM((3, height, LANES), jnp.int32),
        pltpu.VMEM((4, kinds, blocks), jnp.int32),
        pltpu.VMEM((8, kinds, blocks), jnp.float32),
        pltpu.SMEM((3, height, LANES), jnp.int32),
        pltpu.SemaphoreType.DMA,
        pltpu.VMEM((2 * PAIR, 4, LANES), jnp.float32),
        pltpu.VMEM((spare + 1, TILE, 48), jnp.bfloat16),
        pltpu.VMEM((spare + 1, TILE, LANES), jnp.float32),
        pltpu.VMEM((2 * PAIR, TILE, LANES), jnp.float32),
        pltpu.VMEM((PAIR, TILE, 2 * LANES), jnp.bfloat16),
        pltpu.VMEM((2 * PAIR, 16, LANES), jnp.bfloat16),
        pltpu.VMEM((PAIR, 16, LANES), jnp.bfloat16),
        pltpu.VMEM((2 * PAIR, 16, LANES), jnp.bfloat16),
        pltpu.VMEM((2 * PAIR, 16, LANES), jnp.bfloat16),
    ]
    vmem = pl.BlockSpec(memory_space=pltpu.VMEM)
    return pl.pallas_call(
        pull_kernel,
        out_shape=jax.ShapeDtypeStruct((3, blocks, width), jnp.float32),
        in_specs=[vmem] * 6,
        out_specs=vmem,
        scratch_shapes=scratch,
        compiler_params=pltpu.CompilerParams(vmem_limit_bytes=36 * 1024 * 1024),
    )(meta, counts, pos, ranks, sinks, table)


def local(
    positions,
    time_bins,
    home_groups,
    targets,
    target_groups,
    node_pos,
    node_mass,
    node_lists,
    list_counts,
):
    domains = lax.axis_size("dom")
    sharers = lax.axis_size("sub")
    devices = domains * sharers
    blocks, most = targets.shape
    width = positions.shape[2]
    groups, length = node_lists.shape
    share = groups // sharers
    stride = share * 8 + 8
    per_device = node_mass.shape[0]
    height = per_device // LANES
    f32, i32 = jnp.float32, jnp.int32
    vmem = pl.BlockSpec(memory_space=pltpu.VMEM)
    dma = pltpu.SemaphoreType.DMA

    hbm = pl.BlockSpec(memory_space=pltpu.HBM)
    deep, wide = domains // 2, sharers // 2
    most_first = max(2, wide)
    table, counts, ranks, meta, pos, sinks = pl.pallas_call(
        functools.partial(domain_kernel, groups=groups, share=share, stride=stride),
        out_shape=[
            jax.ShapeDtypeStruct((devices, stride, LANES), f32),
            jax.ShapeDtypeStruct((devices, LANES), i32),
            jax.ShapeDtypeStruct((blocks, width), i32),
            jax.ShapeDtypeStruct((2 * most + 3, blocks), i32),
            jax.ShapeDtypeStruct((3, blocks, width), f32),
            jax.ShapeDtypeStruct((blocks, TILE, 48), jnp.bfloat16),
        ],
        in_specs=[hbm] * 9,
        out_specs=[vmem] * 6,
        scratch_shapes=[
            pltpu.VMEM((3, per_device), f32),
            pltpu.VMEM((height, LANES), f32),
            pltpu.VMEM((blocks, width), i32),
            pltpu.VMEM((1, blocks), i32),
            pltpu.VMEM((most, blocks), i32),
            pltpu.VMEM((most, blocks), i32),
            pltpu.VMEM((groups, length), i32),
            pltpu.VMEM((sharers, 3, per_device), f32),
            pltpu.VMEM((sharers, height, LANES), f32),
            pltpu.VMEM((sharers * height * 4, LANES), f32),
            pltpu.VMEM((stride, LANES), f32),
            pltpu.SMEM((groups,), i32),
            dma((9,)),
        ]
        + [dma((2, sharers - 1))] * 2
        + [dma((deep,))] * 2
        + [dma((deep, deep))]
        + [dma((deep, most_first))] * 2
        + [dma((deep, most_first, most_first))] * 2
        + [dma((deep, 2, wide))] * 2,
        compiler_params=pltpu.CompilerParams(
            collective_id=0, has_side_effects=True, vmem_limit_bytes=24 * 1024 * 1024
        ),
    )(
        *(
            pltpu.with_memory_space_constraint(array, pltpu.HBM)
            for array in (
                node_pos,
                node_mass.reshape(height, LANES),
                time_bins,
                home_groups.reshape(1, blocks),
                targets.T,
                target_groups.T,
                node_lists,
                jnp.transpose(positions, (1, 0, 2)),
                list_counts,
            )
        )
    )
    forces = pull_call(
        meta,
        counts,
        pos,
        ranks,
        sinks,
        table.reshape(-1, LANES),
    )
    return jnp.transpose(forces, (1, 0, 2))


def solution(mesh):
    return jax.shard_map(
        local,
        mesh=mesh,
        in_specs=(
            P(("dom", "sub"), None, None),
            P(("dom", "sub"), None),
            P(("dom", "sub")),
            P(("dom", "sub"), None),
            P(("dom", "sub"), None),
            P(None, ("dom", "sub")),
            P(("dom", "sub")),
            P("dom", None),
            P("dom"),
        ),
        out_specs=P(("dom", "sub"), None, None),
        check_vma=False,
    )
```

```python
import functools
import math

import jax
import jax.numpy as jnp
from jax import lax
from jax.experimental import pallas as pl
from jax.experimental.pallas import tpu as pltpu
from jax.sharding import PartitionSpec as P

CUR_BIN = 2
SOFTEN_SQ = 0.04
LANES = 128
SCALE = math.sqrt(math.log2(math.e) / 4)
KAPPA = 0.49
LEAD = 1.064481380238203
POLY = (
    0.6921288825590801,
    -0.08983655460543045,
    -0.026659970636641404,
    0.007383673416911636,
)
MASS_SCALE = LEAD * SCALE / math.sqrt(math.pi)
MESH = pl.DeviceIdType.MESH
TILE = 144
PAIR = 3


def bf16_pieces(value):
    pieces = []
    for _ in range(3):
        mantissa, exponent = math.frexp(value)
        piece = math.ldexp(round(mantissa * 256), exponent - 8)
        pieces.append(piece)
        value -= piece
    return tuple(pieces)


SOFT = bf16_pieces(SOFTEN_SQ * SCALE * SCALE)


def split(value):
    high = value.astype(jnp.bfloat16).astype(jnp.float32)
    rest = value - high
    middle = rest.astype(jnp.bfloat16).astype(jnp.float32)
    return value, rest, rest - middle


def axes(first, second, third, fourth, at):
    return jnp.where(at == 0, first, jnp.where(at == 1, second, jnp.where(at == 2, third, fourth)))


def soft_row():
    lane48 = lax.broadcasted_iota(jnp.int32, (TILE, 48), 1)
    soft_high, soft_rest, soft_last = SOFT
    return jnp.where(
        lane48 == 11,
        soft_high,
        jnp.where(lane48 == 27, soft_rest, jnp.where(lane48 == 43, soft_last, 0.0)),
    )


def block_sinks(pos, ranks, block, tile):
    width = pos.shape[2]
    f32, bf16 = jnp.float32, jnp.bfloat16
    sub8 = lax.broadcasted_iota(jnp.int32, (8, width), 0)
    axis8 = sub8 & 3
    order = lax.broadcasted_iota(jnp.int32, (TILE, width), 0)
    line = [
        jnp.broadcast_to(pos[axis, pl.ds(block, 1), :] * SCALE, (8, width))
        for axis in range(3)
    ]
    norm = line[0] * line[0] + line[1] * line[1] + line[2] * line[2]
    pieces = split(axes(line[0], line[1], line[2], 0.0, axis8) * -2.0)
    norms = split(norm)
    parts = []
    for k in range(3):
        tail = jnp.where(sub8 == 7, norms[k], 1.0 if k == 0 else 0.0)
        parts.append(pieces[k])
        parts.append(jnp.where(sub8 < 3, pieces[k], jnp.where(sub8 == 3, 0.0, tail)))
    wide = jnp.concatenate(parts, axis=0).astype(bf16)
    rank = ranks[pl.ds(block, 1), :]
    pick = jnp.where(order == rank - tile * TILE, 1.0, 0.0).astype(bf16)
    held = lax.dot_general(
        pick, wide, (((1,), (1,)), ((), ())), preferred_element_type=f32
    )
    return (held + soft_row()).astype(bf16)


def fill_ranks(bins, ranks, meta):
    blocks, width = bins.shape
    last = meta.shape[0] - 1
    active = bins[...] <= CUR_BIN
    flags = jnp.where(active, 1.0, 0.0).astype(jnp.bfloat16)
    upper = lax.broadcasted_iota(jnp.int32, (width, width), 0) <= lax.broadcasted_iota(
        jnp.int32, (width, width), 1
    )
    running = jnp.dot(
        flags,
        jnp.where(upper, 1.0, 0.0).astype(jnp.bfloat16),
        preferred_element_type=jnp.float32,
    ).astype(jnp.int32)
    ranks[...] = jnp.where(active, running - 1, -1)
    number = lax.dot_general(
        jnp.ones((8, width), jnp.bfloat16),
        flags,
        (((1,), (1,)), ((), ())),
        preferred_element_type=jnp.float32,
    ).astype(jnp.int32)
    meta[last : last + 1] = number[0:1]


def fill_places(homes, targets, target_groups, meta, groups, share, stride):
    domain = lax.axis_index("dom")
    most = targets.shape[0]
    holders = groups // share

    def places(owner, group):
        slot = owner * holders + lax.div(group, share)
        inner = lax.rem(group, share)
        return slot * LANES + inner, slot * stride + inner * 8

    key, line = places(domain, homes[...])
    meta[0:1] = key
    meta[most + 1 : most + 2] = line
    key, line = places(jnp.maximum(targets[...], 0), target_groups[...])
    meta[1 : most + 1] = jnp.where(targets[...] >= 0, key, LANES - 1)
    meta[most + 2 : 2 * most + 2] = line


def gather_lists(all_pos, all_mass, lists, list_counts, out, stack):
    sharers, _, per_device = all_pos.shape
    height = per_device // LANES
    total, length = lists.shape
    share = total // sharers
    place = lax.axis_index("sub")
    f32, bf16 = jnp.float32, jnp.bfloat16
    for owner in range(sharers):
        for high in range(height):
            at = (owner * height + high) * 4
            stack[at : at + 3] = all_pos[owner, :, high * LANES : (high + 1) * LANES] * SCALE
            stack[at + 3 : at + 4] = all_mass[owner, high : high + 1, :] * MASS_SCALE
    half = sharers * height // 2
    rows = half * 4
    pieces = [
        piece.astype(bf16)
        for piece in split(jnp.concatenate([stack[0:rows], stack[rows : 2 * rows]], axis=1))
    ]
    order = lax.broadcasted_iota(jnp.int32, (2 * LANES, length), 0)
    pair = lax.broadcasted_iota(jnp.int32, (8, length), 0) >> 2
    lane = lax.broadcasted_iota(jnp.int32, (4, length), 1)
    axis = lax.broadcasted_iota(jnp.int32, (4, length), 0)

    def one(local):
        group = place * share + local
        index = lists[pl.ds(group, 1), :]
        high = index >> 7
        far = jnp.where(high >= half, 1, 0)
        low = (index & (LANES - 1)) + far * LANES
        high = jnp.broadcast_to(high - far * half, (8, length)) - pair
        pick = jnp.where(order == low, 1.0, 0.0).astype(bf16)
        found = sum(jnp.dot(piece, pick, preferred_element_type=f32) for piece in pieces)
        total = jnp.zeros((8, length), f32)
        for t in range(rows // 8):
            total = jnp.where(high == 2 * t, found[8 * t : 8 * t + 8], total)
        picked = total[0:4] + total[4:8]
        valid = (axis < 3) | (lane < list_counts[group])
        picked = jnp.where(valid, picked, 0.0)
        out[pl.ds(pl.multiple_of(local * 8, 8), 8), :] = jnp.concatenate(
            [picked[:, 0:LANES], picked[:, LANES : 2 * LANES]], axis=0
        )

    batch = math.gcd(share, 4)

    def some(step, carry):
        for k in range(batch):
            one(step * batch + k)
        return carry

    lax.fori_loop(0, share // batch, some, 0)
    lane8 = lax.broadcasted_iota(jnp.int32, (8, LANES), 1)
    tail = jnp.zeros((8, LANES), jnp.int32)
    for local in range(share):
        tail = jnp.where(lane8 == local, list_counts[place * share + local], tail)
    out[share * 8 : share * 8 + 8, :] = tail.astype(f32)


def domain_kernel(
    node_pos, node_mass, bins, homes, targets, target_groups, lists, positions, list_counts,
    out, counts, ranks, meta, pos, sinks,
    own_pos, own_mass, own_bins, own_homes, own_targets, own_groups, own_lists,
    all_pos, all_mass, stack, own, own_counts,
    load_sem, s_send, s_recv, z_send, z_recv, f_send, p_send, p_recv, q_send, q_recv,
    n_send, n_recv, groups, share, stride,
):
    sharers, domains = lax.axis_size("sub"), lax.axis_size("dom")
    domain, place = lax.axis_index("dom"), lax.axis_index("sub")
    deep, wide = domains // 2, sharers // 2
    half = deep // 2
    core = lax.rem(place, 2)
    across = place // 2
    layer, side = domain // 2, lax.rem(domain, 2)
    upper = layer // half
    gate = (1 - upper) * half + upper * (half - 1)
    other_gate = (1 - upper) * (half - 1) + upper * half
    sibling = {"sub": place + 1 - 2 * core}
    barrier = pltpu.get_barrier_semaphore()

    def shifted(at, by, size):
        return lax.rem(at + by + size, size)

    def device(z, dy, dx):
        return {
            "dom": z * 2 + shifted(side, dy, 2),
            "sub": shifted(across, dx, wide) * 2 + core,
        }

    def slot(z, dy, dx):
        there = device(z, -dy, -dx)
        return there["dom"] * sharers + there["sub"]

    others = [{"sub": lax.rem(place + k, sharers)} for k in range(1, sharers)]
    peers = [device(shifted(layer, k, deep), 0, 0) for k in range(1, deep)]
    peers += [device(layer, 1, 0)] + others
    for peer in peers:
        pl.semaphore_signal(barrier, inc=1, device_id=peer, device_id_type=MESH)
    loads = [
        pltpu.make_async_copy(source, target, load_sem.at[k])
        for k, (source, target) in enumerate(
            (
                (node_pos, own_pos),
                (node_mass, own_mass),
                (bins, own_bins),
                (homes, own_homes),
                (targets, own_targets),
                (target_groups, own_groups),
                (lists, own_lists),
                (positions, pos),
                (list_counts, own_counts),
            )
        )
    ]
    for load in loads:
        load.start()
    for load in loads[:2]:
        load.wait()
    pl.semaphore_wait(barrier, len(peers))
    copies = []
    for k, other in enumerate(others):
        for j, (source, target) in enumerate(((own_pos, all_pos), (own_mass, all_mass))):
            share_copy = pltpu.make_async_remote_copy(
                src_ref=source,
                dst_ref=target.at[place],
                send_sem=s_send.at[j, k],
                recv_sem=s_recv.at[j, k],
                device_id=other,
                device_id_type=MESH,
            )
            share_copy.start()
            copies.append(share_copy)
    all_pos[place] = own_pos[...]
    all_mass[place] = own_mass[...]
    for load in loads[2:]:
        load.wait()
    fill_ranks(own_bins, ranks, meta)

    def prepare(step, carry):
        for k in range(4):
            sinks[step * 4 + k] = block_sinks(pos, ranks, step * 4 + k, 0)
        return carry

    lax.fori_loop(0, sinks.shape[0] // 4, prepare, 0)
    for share_copy in copies:
        share_copy.wait_recv()
    gather_lists(all_pos, all_mass, own_lists, own_counts, own, stack)
    fill_places(own_homes, own_targets, own_groups, meta, groups, share, stride)

    def run(side_first):
        first, second = (2, wide) if side_first else (wide, 2)

        def cell(j, i):
            return (j, i) if side_first else (i, j)

        def copy(source, at, send, recv, there):
            return pltpu.make_async_remote_copy(
                src_ref=source,
                dst_ref=out.at[at],
                send_sem=send,
                recv_sem=recv,
                device_id=there,
                device_id_type=MESH,
            )

        mine = slot(layer, 0, 0)

        def z_copy(k, to):
            return copy(own, mine, z_send.at[k], z_recv.at[layer], device(to, 0, 0))

        def z_wait(z):
            copy(own, slot(z, 0, 0), z_send.at[0], z_recv.at[z], device(z, 0, 0)).wait_recv()

        def f_copy(z, k):
            to = upper * half + lax.rem(layer - upper * half + k, half)
            at = slot(z, 0, 0)
            return copy(
                out.at[at], at, f_send.at[lax.rem(z, half), k], z_recv.at[z], device(to, 0, 0)
            )

        def p_copy(z, j, source=None):
            at = slot(z, 0, 0)
            return copy(
                out.at[at] if source is None else source,
                at,
                p_send.at[z, j],
                p_recv.at[z, j],
                device(layer, *cell(j, 0)),
            )

        def q_copy(z, j, i, source=None):
            at = slot(z, *cell(j, 0))
            return copy(
                out.at[at] if source is None else source,
                at,
                q_send.at[z, j, i],
                q_recv.at[z, j, i],
                device(layer, *cell(0, i)),
            )

        def n_copy(z, j, i, source=None):
            c = cell(j, i)
            at = slot(z, *c)
            return copy(
                out.at[at] if source is None else source,
                at,
                n_send.at[(z,) + c],
                n_recv.at[(z,) + c],
                sibling,
            )

        def after_z(z, source=None):
            for j in range(1, first):
                p_copy(z, j, source).start()
            for i in range(1, second):
                q_copy(z, 0, i, source).start()
            n_copy(z, 0, 0, source).start()

        def take_z(z):
            z_wait(z)

            @pl.when((layer == other_gate) & (z // half != upper))
            def _():
                for k in range(1, half):
                    f_copy(z, k).start()

            after_z(z)

        def take_p(z):
            for j in range(1, first):
                p_copy(z, j).wait_recv()
                for i in range(1, second):
                    q_copy(z, j, i).start()
                n_copy(z, j, 0).start()

        def take_q(z):
            for j in range(first):
                for i in range(1, second):
                    q_copy(z, j, i).wait_recv()
                    n_copy(z, j, i).start()

        def at_distance(k, action):
            pl.when(layer + k < deep)(lambda: action(layer + k))
            pl.when(layer - k >= 0)(lambda: action(layer - k))

        for k in range(1, half):
            z_copy(k, upper * half + lax.rem(layer - upper * half + k, half)).start()
        z_copy(0, gate).start()
        after_z(layer, own)
        out[mine] = own[...]
        take_p(layer)
        for k in range(1, deep):
            at_distance(k, take_z)
            if k > 1:
                at_distance(k - 1, take_p)
        at_distance(deep - 1, take_p)
        take_q(layer)
        for k in range(1, deep):
            at_distance(k, take_q)
        for k in range(half):
            z_copy(k, gate).wait_send()

        @pl.when(layer == other_gate)
        def _():
            for z in range(half):
                for k in range(1, half):
                    f_copy(z, k).wait_send()

        for z in range(deep):
            for j in range(first):
                for i in range(second):
                    if i == 0 and j > 0:
                        p_copy(z, j).wait_send()
                    if i > 0:
                        q_copy(z, j, i).wait_send()
                    n_copy(z, j, i).wait()

    pl.when(core == 0)(lambda: run(True))
    pl.when(core == 1)(lambda: run(False))
    for share_copy in copies:
        share_copy.wait_send()
    tail = out.shape[1] - 8
    counts[...] = out[:, tail, :].astype(jnp.int32)


def radial(range_sq):
    near = lax.rsqrt(range_sq)
    fall = 1.0 / (range_sq * jnp.exp2(range_sq))
    z = 1.0 / (near + KAPPA)
    poly = z * POLY[-1] + POLY[-2]
    for coefficient in POLY[-3::-1]:
        poly = poly * z + coefficient
    return (poly * z + near) * fall


def compact(rows, places, wide):
    order = lax.broadcasted_iota(jnp.int32, (wide, wide), 0)
    pick = jnp.where(order == places, 1.0, 0.0).astype(jnp.bfloat16)
    return lax.dot_general(
        rows.astype(jnp.bfloat16),
        pick,
        (((1,), (1,)), ((), ())),
        preferred_element_type=jnp.float32,
    )


def plan_items(meta, counts, plan, fields, pieces, tiles):
    f32, bf16, i32 = jnp.float32, jnp.bfloat16, jnp.int32
    blocks = meta.shape[1]
    visits = (meta.shape[0] - 1) // 2
    slots = counts.shape[0]
    height = plan.shape[1]
    spare = tiles * blocks
    held = counts[...].astype(f32).astype(bf16)
    order = lax.broadcasted_iota(i32, (LANES, blocks), 0)
    slot = lax.broadcasted_iota(i32, (slots, blocks), 0)
    active = meta[2 * visits : 2 * visits + 1]
    full, ends, lines = [], [], []
    for visit in range(visits):
        key = meta[visit : visit + 1]
        pick = jnp.where(order == (key & (LANES - 1)), 1.0, 0.0).astype(bf16)
        found = jnp.dot(held, pick, preferred_element_type=f32)
        count = jnp.sum(jnp.where(slot == (key >> 7), found, 0.0), axis=0, keepdims=True)
        count = count.astype(i32)
        line = meta[visits + visit : visits + visit + 1]
        more = count > LANES
        full.append((jnp.where(more, 1, 0), line, line, jnp.full_like(line, LANES)))
        ends.append(jnp.where(more, count - LANES, count))
        lines.append(jnp.where(more, line + 4, line))
    entries = list(full)
    size, at = ends[0], lines[0]
    for visit in range(1, visits):
        end, line = ends[visit], lines[visit]
        both = jnp.minimum(size, 1) * jnp.minimum(end, 1)
        fit = jnp.where(size + end <= LANES, both, 0)
        bigger = end > size
        entries.append(
            (
                both,
                jnp.where((fit == 0) & bigger, line, at),
                line,
                jnp.where(fit > 0, size, LANES),
            )
        )
        take = jnp.where(both > 0, jnp.where(bigger, 0, 1), jnp.where(end > 0, 1, 0))
        at = jnp.where(take > 0, line, at)
        size = jnp.where(fit > 0, 0, jnp.where(take > 0, end, size))
    entries.append((jnp.minimum(size, 1), at, at, jnp.full_like(at, LANES)))
    kinds = len(entries)
    used = kinds * tiles
    for k in range(4):
        fields[k] = jnp.zeros(fields.shape[1:], i32)
    for tile in range(tiles):
        live = jnp.where(active > tile * TILE, 1, 0)
        for j, entry in enumerate(entries):
            row = tile * kinds + j
            fields[0, row : row + 1] = entry[0] * live if tile > 0 else entry[0]
            for k in range(1, 4):
                fields[k, row : row + 1] = entry[k]
    valid = fields[0].astype(f32).astype(bf16)
    below = lax.broadcasted_iota(i32, (blocks, blocks), 0) < lax.broadcasted_iota(
        i32, (blocks, blocks), 1
    )
    below = jnp.where(below, 1.0, 0.0).astype(bf16)
    before = jnp.dot(valid, below, preferred_element_type=f32)
    sums = jnp.dot(valid, jnp.ones((blocks, blocks), bf16), preferred_element_type=f32)
    tall = fields.shape[1]
    under = lax.broadcasted_iota(i32, (tall, tall), 0) > lax.broadcasted_iota(
        i32, (tall, tall), 1
    )
    under = jnp.where(under, 1.0, 0.0).astype(bf16)
    start = jnp.dot(under, sums.astype(bf16), preferred_element_type=f32)
    place = (start + before).astype(i32)
    number = jnp.sum(sums, axis=0, keepdims=True).astype(i32)
    first, second = fields[1], fields[2]
    block_at = lax.broadcasted_iota(i32, (tall, blocks), 1)
    parts = (
        first & 255,
        first >> 8,
        second & 255,
        second >> 8,
        fields[3],
        block_at,
        place // blocks,
        jnp.ones_like(place),
    )
    for k, part in enumerate(parts):
        pieces[k] = part.astype(f32)
    lane = lax.rem(place, blocks)
    fields[0] = jnp.where(fields[0] > 0, lane, -1)
    row = lax.broadcasted_iota(i32, (height, blocks), 0)
    words = [jnp.full((height, blocks), spare * 65536, i32), jnp.zeros((height, blocks), i32)]
    for r in range(used):
        got = compact(pieces[:, r, :], fields[0, r : r + 1], blocks).astype(i32)
        one = got[0:1] + got[1:2] * 256 + (got[5:6] + r // kinds * blocks) * 65536
        two = got[2:3] + got[3:4] * 256 + got[4:5] * 65536
        here = jnp.where(got[7:8] > 0, got[6:7], -1) == row
        words = [jnp.where(here, one, words[0]), jnp.where(here, two, words[1])]
    plan[0, :, 0:blocks] = words[0]
    plan[1, :, 0:blocks] = words[1]
    plan[2, 0:1, 0:blocks] = number
    numbers = lax.broadcasted_iota(i32, (8, blocks), 1).astype(f32)
    for tile in range(1, tiles):
        live = jnp.where(active > tile * TILE, 1.0, 0.0)
        rows = jnp.broadcast_to(live, (8, blocks)).astype(bf16)
        spot = jnp.dot(rows, below, preferred_element_type=f32)[0:1].astype(i32)
        got = compact(numbers, jnp.where(live > 0, spot, -1), blocks).astype(i32)
        total = jnp.dot(rows, jnp.ones((blocks, blocks), bf16), preferred_element_type=f32)
        plan[2, 2 * tile - 1 : 2 * tile, 0:blocks] = got[0:1]
        plan[2, 2 * tile : 2 * tile + 1, 0:blocks] = total[0:1].astype(i32)


def pull_kernel(
    meta, counts, pos, ranks, own_sinks, table, out,
    plan, fields, pieces, items, plan_sem, mixed, sinks, totals,
    later_range, later_weight, later_nodes, last_nodes, next_group, next_nodes,
):
    blocks = meta.shape[1]
    width = pos.shape[2]
    tiles = sinks.shape[0] // blocks
    spare = tiles * blocks
    f32, bf16 = jnp.float32, jnp.bfloat16
    by_rows = (((1,), (1,)), ((), ()))

    def prepare(block, tile):
        at = tile * blocks + block
        sinks[at] = block_sinks(pos, ranks, block, tile)
        totals[at] = jnp.zeros((TILE, LANES), f32)

    def first(step, carry):
        for k in range(4):
            block = step * 4 + k
            sinks[block] = own_sinks[block]
            totals[block] = jnp.zeros((TILE, LANES), f32)
        return carry

    plan_items(meta, counts, plan, fields, pieces, tiles)
    sinks[spare] = soft_row().astype(bf16)
    totals[spare] = jnp.zeros((TILE, LANES), f32)
    move = pltpu.make_async_copy(plan, items, plan_sem)
    lax.fori_loop(0, 2, first, 0)
    move.start()
    lax.fori_loop(2, blocks // 4, first, 0)
    move.wait()
    number = items[2, 0, 0]

    def beyond(tile, action):
        def one(step, carry):
            action(items[2, 2 * tile - 1, step], tile)
            return carry

        lax.fori_loop(0, items[2, 2 * tile, 0], one, 0)

    for tile in range(1, tiles):
        beyond(tile, prepare)

    sub = lax.broadcasted_iota(jnp.int32, (8, LANES), 0)
    axis = sub & 3

    lane4 = lax.broadcasted_iota(jnp.int32, (4, LANES), 1)
    bits = blocks.bit_length() - 1
    assert blocks == 1 << bits

    def word(kind, item):
        return items[kind, lax.shift_right_logical(item, bits), item & (blocks - 1)]

    def begin(item, spot):
        code, other = word(0, item), word(1, item)
        shift = other >> 16
        moved = pltpu.roll(table[pl.ds(other & 65535, 4), :], shift & (LANES - 1), 1)
        mixed[spot] = jnp.where(lane4 < shift, table[pl.ds(code & 65535, 4), :], moved)
        row = [jnp.broadcast_to(mixed[spot, f : f + 1, :], (8, LANES)) for f in range(4)]
        norm = row[0] * row[0] + row[1] * row[1] + row[2] * row[2]
        flat = axes(row[0], row[1], row[2], row[3], axis)
        pieces = split(flat)
        norms = split(norm)
        tail = jnp.where(
            sub == 4, norms[0], jnp.where(sub == 5, norms[1], jnp.where(sub == 6, norms[2], 1.0))
        )
        group = jnp.concatenate(
            [
                jnp.where(sub < 4, pieces[0], pieces[1]),
                jnp.where(sub < 3, pieces[2], tail),
            ],
            axis=0,
        ).astype(bf16)
        weighted = split(jnp.where(axis == 3, flat, flat * row[3]))
        moment = jnp.concatenate(
            [
                jnp.where(sub < 4, weighted[0], weighted[1]),
                jnp.where(sub < 4, weighted[2], 0.0),
            ],
            axis=0,
        ).astype(bf16)
        return group, moment

    def reach(item, spot):
        group = next_group[spot]
        return jnp.dot(
            sinks[word(0, item) >> 16],
            jnp.concatenate([group] * 3, axis=0),
            preferred_element_type=f32,
        )

    def weigh(range_sq):
        weight = radial(range_sq)
        high = weight.astype(bf16)
        low = (weight - high.astype(f32)).astype(bf16)
        return jnp.concatenate([high, low], axis=1)

    def gather(weight, moment):
        moment = jnp.concatenate([moment] * 2, axis=1)
        return lax.dot_general(weight, moment, by_rows, preferred_element_type=f32)

    def add(item, pull):
        at = word(0, item) >> 16
        totals[at, :, 0:16] += pull

    for k in range(2 * PAIR):
        next_group[k], later_nodes[k] = begin(k, k)
    for k in range(2 * PAIR):
        later_range[k] = reach(k, k)
    for k in range(2 * PAIR):
        next_group[k], next_nodes[k] = begin(2 * PAIR + k, k)
    for k in range(PAIR):
        later_weight[k] = jnp.zeros(later_weight.shape[1:], bf16)
        last_nodes[k] = jnp.zeros(last_nodes.shape[1:], bf16)

    def main(step, carry):
        base = step * (2 * PAIR)
        before = [gather(later_weight[k], last_nodes[k]) for k in range(PAIR)]
        after = [reach(base + 2 * PAIR + k, k) for k in range(2 * PAIR)]
        now = [gather(weigh(later_range[k]), later_nodes[k]) for k in range(PAIR)]
        for k in range(PAIR):
            add(jnp.where(step > 0, base - PAIR + k, number), before[k])
        for k in range(PAIR):
            later_weight[k] = weigh(later_range[PAIR + k])
            last_nodes[k] = later_nodes[PAIR + k]
        for k in range(PAIR):
            add(base + k, now[k])
        fresh = [begin(base + 4 * PAIR + k, k) for k in range(2 * PAIR)]
        for k in range(2 * PAIR):
            later_range[k] = after[k]
            later_nodes[k] = next_nodes[k]
            next_group[k], next_nodes[k] = fresh[k]
        return carry

    groups = (number + PAIR - 1) // PAIR
    lax.fori_loop(0, groups // 2 + 1, main, 0)

    lane16 = lax.broadcasted_iota(jnp.int32, (TILE, LANES), 1)
    wide_tile = -(-TILE // LANES) * LANES

    def laid(flat, block, tile):
        flat = flat[0:4] + flat[4:8] + flat[8:12]
        flat = jnp.concatenate([flat, flat], axis=0)
        rank = jnp.broadcast_to(ranks[pl.ds(block, 1), :] - tile * TILE, (8, width))
        parts = []
        for k in range(0, width, LANES):
            at = rank[:, k : k + LANES]
            low = at & (LANES - 1)
            part = jnp.zeros((8, LANES), f32)
            for j in range(0, wide_tile, LANES):
                piece = jnp.take_along_axis(
                    flat[:, j : j + LANES], low, axis=1, mode="promise_in_bounds"
                )
                here = (at >= j) & (at < min(j + LANES, TILE))
                part = jnp.where(here, piece, part)
            parts.append(part)
        return jnp.concatenate(parts, axis=1)

    def turn(value):
        value = jnp.concatenate(
            [value, jnp.zeros((wide_tile - TILE, LANES), f32)], axis=0
        )
        return jnp.transpose(value)

    def store(block, sums):
        for axis in range(3):
            there = pos[axis, pl.ds(block, 1), :] * SCALE
            out[axis, pl.ds(block, 1), :] = sums[axis : axis + 1] - sums[3:4] * there

    def last(step, carry):
        packed = totals[step * 8]
        for k in range(1, 8):
            moved = pltpu.roll(totals[step * 8 + k], 16 * k, 1)
            packed = jnp.where(lane16 < 16 * k, packed, moved)
        turned = turn(packed)
        for k in range(8):
            store(step * 8 + k, laid(turned[16 * k : 16 * k + 16], step * 8 + k, 0))
        return carry

    lax.fori_loop(0, blocks // 8, last, 0)

    def rest(block, tile):
        sums = laid(turn(totals[tile * blocks + block])[0:16], block, tile)
        for axis in range(3):
            there = pos[axis, pl.ds(block, 1), :] * SCALE
            out[axis, pl.ds(block, 1), :] += sums[axis : axis + 1] - sums[3:4] * there

    for tile in range(1, tiles):
        beyond(tile, rest)


def pull_call(meta, counts, pos, ranks, sinks, table):
    blocks, width = ranks.shape
    visits = (meta.shape[0] - 1) // 2
    tiles = -(-width // TILE)
    spare = tiles * blocks
    kinds = -(-2 * visits * tiles // 8) * 8
    height = -(-(2 * visits * tiles * blocks + 12 * PAIR) // (8 * blocks)) * 8
    scratch = [
        pltpu.VMEM((3, height, LANES), jnp.int32),
        pltpu.VMEM((4, kinds, blocks), jnp.int32),
        pltpu.VMEM((8, kinds, blocks), jnp.float32),
        pltpu.SMEM((3, height, LANES), jnp.int32),
        pltpu.SemaphoreType.DMA,
        pltpu.VMEM((2 * PAIR, 4, LANES), jnp.float32),
        pltpu.VMEM((spare + 1, TILE, 48), jnp.bfloat16),
        pltpu.VMEM((spare + 1, TILE, LANES), jnp.float32),
        pltpu.VMEM((2 * PAIR, TILE, LANES), jnp.float32),
        pltpu.VMEM((PAIR, TILE, 2 * LANES), jnp.bfloat16),
        pltpu.VMEM((2 * PAIR, 16, LANES), jnp.bfloat16),
        pltpu.VMEM((PAIR, 16, LANES), jnp.bfloat16),
        pltpu.VMEM((2 * PAIR, 16, LANES), jnp.bfloat16),
        pltpu.VMEM((2 * PAIR, 16, LANES), jnp.bfloat16),
    ]
    vmem = pl.BlockSpec(memory_space=pltpu.VMEM)
    return pl.pallas_call(
        pull_kernel,
        out_shape=jax.ShapeDtypeStruct((3, blocks, width), jnp.float32),
        in_specs=[vmem] * 6,
        out_specs=vmem,
        scratch_shapes=scratch,
        compiler_params=pltpu.CompilerParams(vmem_limit_bytes=36 * 1024 * 1024),
    )(meta, counts, pos, ranks, sinks, table)


def local(
    positions,
    time_bins,
    home_groups,
    targets,
    target_groups,
    node_pos,
    node_mass,
    node_lists,
    list_counts,
):
    domains = lax.axis_size("dom")
    sharers = lax.axis_size("sub")
    devices = domains * sharers
    blocks, most = targets.shape
    width = positions.shape[2]
    groups, length = node_lists.shape
    share = groups // sharers
    stride = share * 8 + 8
    per_device = node_mass.shape[0]
    height = per_device // LANES
    f32, i32 = jnp.float32, jnp.int32
    vmem = pl.BlockSpec(memory_space=pltpu.VMEM)
    dma = pltpu.SemaphoreType.DMA

    hbm = pl.BlockSpec(memory_space=pltpu.HBM)
    deep, wide = domains // 2, sharers // 2
    most_first = max(2, wide)
    table, counts, ranks, meta, pos, sinks = pl.pallas_call(
        functools.partial(domain_kernel, groups=groups, share=share, stride=stride),
        out_shape=[
            jax.ShapeDtypeStruct((devices, stride, LANES), f32),
            jax.ShapeDtypeStruct((devices, LANES), i32),
            jax.ShapeDtypeStruct((blocks, width), i32),
            jax.ShapeDtypeStruct((2 * most + 3, blocks), i32),
            jax.ShapeDtypeStruct((3, blocks, width), f32),
            jax.ShapeDtypeStruct((blocks, TILE, 48), jnp.bfloat16),
        ],
        in_specs=[hbm] * 9,
        out_specs=[vmem] * 6,
        scratch_shapes=[
            pltpu.VMEM((3, per_device), f32),
            pltpu.VMEM((height, LANES), f32),
            pltpu.VMEM((blocks, width), i32),
            pltpu.VMEM((1, blocks), i32),
            pltpu.VMEM((most, blocks), i32),
            pltpu.VMEM((most, blocks), i32),
            pltpu.VMEM((groups, length), i32),
            pltpu.VMEM((sharers, 3, per_device), f32),
            pltpu.VMEM((sharers, height, LANES), f32),
            pltpu.VMEM((sharers * height * 4, LANES), f32),
            pltpu.VMEM((stride, LANES), f32),
            pltpu.SMEM((groups,), i32),
            dma((9,)),
        ]
        + [dma((2, sharers - 1))] * 2
        + [dma((deep,))] * 2
        + [dma((deep, deep))]
        + [dma((deep, most_first))] * 2
        + [dma((deep, most_first, most_first))] * 2
        + [dma((deep, 2, wide))] * 2,
        compiler_params=pltpu.CompilerParams(
            collective_id=0, has_side_effects=True, vmem_limit_bytes=24 * 1024 * 1024
        ),
    )(
        *(
            pltpu.with_memory_space_constraint(array, pltpu.HBM)
            for array in (
                node_pos,
                node_mass.reshape(height, LANES),
                time_bins,
                home_groups.reshape(1, blocks),
                targets.T,
                target_groups.T,
                node_lists,
                jnp.transpose(positions, (1, 0, 2)),
                list_counts,
            )
        )
    )
    forces = pull_call(
        meta,
        counts,
        pos,
        ranks,
        sinks,
        table.reshape(-1, LANES),
    )
    return jnp.transpose(forces, (1, 0, 2))


def solution(mesh):
    return jax.shard_map(
        local,
        mesh=mesh,
        in_specs=(
            P(("dom", "sub"), None, None),
            P(("dom", "sub"), None),
            P(("dom", "sub")),
            P(("dom", "sub"), None),
            P(("dom", "sub"), None),
            P(None, ("dom", "sub")),
            P(("dom", "sub")),
            P("dom", None),
            P("dom"),
        ),
        out_specs=P(("dom", "sub"), None, None),
        check_vma=False,
    )
```
